32 devices in a mesh: row: 8 (over z, y), col: 4 (over x, core).
Axes of the slice: x: 2, y: 2, z: 4, core: 2. Of those that a mesh axis runs over, the one named last changes fastest.
Arguments:
- rhs: float32 [2, 8, 64, 512], P(None, 'row'), may hold values from -6 to 6
- inverse_t: float32 [2, 8, 512, 512], P(None, 'row', None, 'col'), may hold values from -1 to 2, as said below
- u_factors: bfloat16 [2, 8, 4, 4, 32, 512], P(None, 'row', None, 'col'), may hold values from -0.14941406 to 0.14941406
- v_factors: bfloat16 [2, 8, 4, 4, 32, 512], P(None, 'row', None, 'col'), may hold values from -0.14941406 to 0.14941406
- tile_ranks: int32 [2, 8, 4, 4], P(None, 'row', None, 'col'), may hold values from 8 to 32
Outputs:
- solved: float32 [2, 8, 64, 512], P(None, 'row')
The draws below stay inside these ranges and needn't reach their ends.
Inputs may be any that keep to these rules, and one draw needn't show every extreme that they name: `inverse_t`: each transposed inverse is nonsingular and of order one.
All inputs are finite; a program needn't handle non-finite values.
Results may differ from the reference program's by a relative error of at most 0.004.
Values may be sent and summed in bfloat16 or wider, within the bound.
No kernel may reach another device: no remote copies, remote signals or barrier semaphores. Data moves between devices by JAX's collectives and lax.ppermute only.
A program may use at most 64 MiB of HBM per device.

```python
import jax
import jax.numpy as jnp
from jax import lax

B = 512
R = 64
K = 32
BR = 2
NB = 16
BC = 4
N_ROW = 8
N_COL = 4


def draw_inverse_t(key, part):
    shape = (BR, NB // BR, B, B)
    eye = jnp.eye(B, dtype=jnp.float32)
    noise = jax.random.normal(key, shape, jnp.float32) * (0.5 / B ** 0.5)
    return jnp.clip(eye + noise, -1.0, 2.0)


def plant(result, key, smallest, largest):
    spot = [jax.random.randint(jax.random.fold_in(key, axis), (), 0, length) for axis, length in enumerate(result.shape)]
    longest = result.shape.index(max(result.shape))
    next_to = spot[:longest] + [(spot[longest] + 1) % result.shape[longest]] + spot[longest + 1:]
    return result.at[tuple(spot)].set(smallest).at[tuple(next_to)].set(largest)


def shard_levels(own_key, extent, cuts, low, top_value):
    def one(dim, blocks):
        steps = jax.random.uniform(jax.random.fold_in(jax.random.fold_in(own_key, 6), dim), (blocks,), jnp.float32, low / len(cuts), top_value / len(cuts))
        return jnp.repeat(jnp.exp(steps), extent[dim] // blocks).reshape((-1,) + (1,) * (len(extent) - dim - 1))

    loudness = one(*cuts[0])
    for cut in cuts[1:]:
        loudness = loudness * one(*cut)
    return loudness


def normal_values(own_key, extent, scale, limit, cuts=(), kind=jnp.bfloat16):
    values = scale * jax.random.normal(own_key, extent, jnp.float32)
    if cuts:
        values = values * shard_levels(own_key, extent, cuts, -0.22, 0.18)
    return jnp.clip(values, -limit, limit).astype(kind)


def setup_inputs(seed: int = 0) -> dict:
    seeds = jax.random.split(jax.random.key(seed), 6)
    rhs = normal_values(seeds[0], (BR, N_ROW, R, B), 1.0, 6.0, ((1, 8),), jnp.float32)
    inverse_t = draw_inverse_t(jax.random.fold_in(seeds[5], 71), 0)
    u_factors = normal_values(seeds[2], (BR, N_ROW, BC, N_COL, K, B), 0.025, 0.14941406, ((1, 8), (3, 4)))
    v_factors = normal_values(seeds[3], (BR, N_ROW, BC, N_COL, K, B), 0.025, 0.14941406, ((1, 8), (3, 4)))
    tile_ranks = plant(jax.random.randint(seeds[4], (BR, N_ROW, BC, N_COL), K // 4, K + 1), jax.random.fold_in(seeds[4], 1), K // 4, K).astype(jnp.int32)
    return dict(rhs=rhs, inverse_t=inverse_t, u_factors=u_factors, v_factors=v_factors, tile_ranks=tile_ranks)


def pick(array, index, axis):
    return lax.dynamic_index_in_dim(array, index, axis, keepdims=False)


def reference(rhs, inverse_t, u_factors, v_factors, tile_ranks):
    blocks = BR * N_ROW
    global_rows = (jnp.arange(BR, dtype=jnp.int32)[:, None] * N_ROW + jnp.arange(N_ROW, dtype=jnp.int32)[None, :])
    rank_cols = jnp.arange(K, dtype=jnp.int32)

    def step(k, carry):
        totals, solved = carry
        k = jnp.asarray(k).astype(jnp.int32)
        k_slot = (k // N_ROW).astype(jnp.int32)
        k_row = (k % N_ROW).astype(jnp.int32)
        c_slot = (k // N_COL).astype(jnp.int32)
        c_dev = (k % N_COL).astype(jnp.int32)
        segment = pick(pick(rhs, k_slot, 0), k_row, 0) - pick(pick(totals, k_slot, 0), k_row, 0)
        inv_block = pick(pick(inverse_t, k_slot, 0), k_row, 0)
        value = jnp.dot(segment, inv_block, precision=lax.Precision.HIGHEST, preferred_element_type=jnp.float32)
        row_block = pick(solved, k_slot, 0)
        row_block = lax.dynamic_update_index_in_dim(row_block, value, k_row, 0)
        solved = lax.dynamic_update_index_in_dim(solved, row_block, k_slot, 0)
        seg_b = value.astype(jnp.bfloat16).astype(jnp.float32)
        v_col = pick(pick(v_factors, c_slot, 2), c_dev, 2).astype(jnp.float32)
        u_col = pick(pick(u_factors, c_slot, 2), c_dev, 2).astype(jnp.float32)
        ranks = pick(pick(tile_ranks, c_slot, 2), c_dev, 2)
        proj = jnp.einsum("rb,xykb->xyrk", seg_b, v_col)
        keep = (rank_cols[None, None, None, :] < ranks[:, :, None, None]) & (global_rows > k)[:, :, None, None]
        proj_b = jnp.where(keep, proj, 0.0).astype(jnp.bfloat16).astype(jnp.float32)
        update = jnp.einsum("xyrk,xykb->xyrb", proj_b, u_col)
        return totals + update, solved

    start = jnp.zeros(rhs.shape, jnp.float32)
    totals, solved = lax.fori_loop(0, blocks, step, (start, start))
    return solved
```

```python
import functools

import jax
import jax.numpy as jnp
from jax import lax
from jax.experimental import pallas as pl
from jax.experimental.pallas import tpu as pltpu
from jax.sharding import PartitionSpec as P

BF = jnp.bfloat16
F32 = jnp.float32
NT = (((1,), (1,)), ((), ()))
TN = (((0,), (0,)), ((), ()))


def mm(a, b):
    return jnp.dot(a, b, preferred_element_type=F32)


def split_mm(a, b):
    high = a.astype(BF)
    low = (a - high.astype(F32)).astype(BF)
    return mm(high, b) + mm(low, b)


def pack(low, high, both, half):
    return jnp.concatenate([high[:, :half], jnp.where(both, low[:, :half], high[:, half:])], axis=1)


def first_kernel(dims, here_ref, rhs_ref, inv_ref, u_ref, v_ref, msg_ref, far_ref):
    n_row, n_col, r_cols, rank, width, half = dims
    row, col = here_ref[0], here_ref[1]
    turn = row // n_col
    inv = inv_ref[...]
    z = split_mm(rhs_ref[...], inv)
    w = mm(u_ref[: (n_row - 1) * rank, :], inv)
    x = jnp.concatenate([z.astype(BF), w.astype(BF)], axis=0)
    near = []
    for t in range(2):
        s = lax.rem(turn - t + 2, 2)
        v = jnp.concatenate([v_ref[s, 0], v_ref[s, 1]], axis=0)
        tile = lax.dot_general(v, x, NT, preferred_element_type=F32).astype(BF)
        near.append(tile[:rank, :width])
        far_ref[t] = tile[rank:]
    msg_ref[...] = pack(near[0], near[1], col > row, half)


def start_solve(q_ref, n_row, r_cols):
    q_ref[...] = jnp.zeros(q_ref.shape, BF)
    eye = (
        lax.broadcasted_iota(jnp.int32, (r_cols, r_cols), 0)
        == lax.broadcasted_iota(jnp.int32, (r_cols, r_cols), 1)
    ).astype(BF)
    for k in range(n_row):
        q_ref[k, :r_cols, :] = eye


def solve(dims, g_ref, q_ref, extra):
    n_row, n_col, r_cols, rank, width, half = dims
    start_solve(q_ref, n_row, r_cols)
    extras = []
    for k in range(n_row):
        parts = []
        w = half if k <= n_col - 2 else width
        for i in range(k + 1, n_row):
            c, t = i % n_col, i // n_col
            at = half if t == 0 else 0
            parts.append(g_ref[k * n_col + c, :, at : at + w])
        if extra is not None:
            if k == n_row - 1:
                w = width + rank
            parts.append(extra(k)[:, :w])
        if not parts:
            break
        a = parts[0] if len(parts) == 1 else jnp.concatenate(parts, axis=0)
        new = mm(a, q_ref[k, :w, :])
        for i in range(k + 1, n_row):
            at = (i - k - 1) * rank
            q_ref[i, r_cols + k * rank : r_cols + (k + 1) * rank, :] = (-new[at : at + rank]).astype(BF)
        if extra is not None:
            extras.append(new[(n_row - 1 - k) * rank :].astype(BF))
    return extras


def middle_kernel(dims, here_ref, g_ref, far_ref, rhs_ref, inv_ref, u_low_ref, u_ref, v_ref, z0_ref, inv0_ref, u0_ref,
                  msg_ref, minus_ref, y_ref, q_ref):
    n_row, n_col, r_cols, rank, width, half = dims
    row, col = here_ref[0], here_ref[1]
    turn = row // n_col
    base = turn * n_col + col
    inv = inv_ref[...]
    w = mm(u_ref[: (n_row - 2) * rank, :], inv)
    p = solve(dims, g_ref, q_ref, lambda k: far_ref[lax.rem(base - k + n_row, n_row)])
    total = lax.dot_general(jnp.concatenate(p, axis=0), u_low_ref[...], TN, preferred_element_type=F32)
    z = split_mm(rhs_ref[...] - total, inv)
    minus_ref[...] = -total
    x = jnp.concatenate([z.astype(BF), w.astype(BF)], axis=0)
    near = []
    for t in range(2):
        s = lax.rem(turn - t + 2, 2)
        near.append(lax.dot_general(v_ref[s, 2], x, NT, preferred_element_type=F32).astype(BF))
    msg_ref[...] = pack(near[0], near[1], col > row, half)
    own = q_ref[row][r_cols:, :]
    minus = lax.dot_general(own, u0_ref[: (n_row - 1) * rank, :], TN, preferred_element_type=F32)
    y_ref[...] = z0_ref[...] + split_mm(minus, inv0_ref[...])


def last_kernel(dims, here_ref, g_ref, minus_ref, inv_ref, u_ref, z_ref, y_ref, q_ref):
    n_row, n_col, r_cols, rank, width, half = dims
    row = here_ref[0]
    solve(dims, g_ref, q_ref, None)
    own = q_ref[row][r_cols:, :]
    minus = minus_ref[...] + lax.dot_general(own, u_ref[: (n_row - 1) * rank, :], TN, preferred_element_type=F32)
    y_ref[...] = z_ref[...] + split_mm(minus, inv_ref[...])


def call(kernel, outs, scratch, *args):
    vmem = pl.BlockSpec(memory_space=pltpu.VMEM)
    return pl.pallas_call(
        kernel,
        out_shape=outs,
        in_specs=[pl.BlockSpec(memory_space=pltpu.SMEM)] + [vmem] * (len(args) - 1),
        out_specs=[vmem] * len(outs),
        scratch_shapes=scratch,
    )(*args)


def on_device(rhs, inverse_t, u_factors, v_factors, tile_ranks):
    slots, _, r_cols, order = rhs.shape
    rank = u_factors.shape[4]
    n_row = lax.axis_size("row")
    n_col = lax.axis_size("col")
    turns = n_row // n_col
    assert slots == 2 and turns == 2 and u_factors.shape[2] == slots * turns
    row = lax.axis_index("row")
    col = lax.axis_index("col")
    here = jnp.stack([row, col]).astype(jnp.int32)
    both = ("row", "col")
    width = r_cols + (n_row - 2) * rank
    half = r_cols + (n_col - 2) * rank
    assert 2 * half == width
    dims = (n_row, n_col, r_cols, rank, width, half)

    rhs_here = rhs[:, 0]
    inv_here = inverse_t[:, 0]
    u_here = u_factors[:, 0, :, 0].reshape(slots, slots, turns, rank, order)
    v_here = v_factors[:, 0, :, 0].reshape(slots, slots, turns, rank, order)
    ranks = tile_ranks[:, 0, :, 0].reshape(slots, slots, turns)
    keep = lax.broadcasted_iota(jnp.int32, v_here.shape, 3) < ranks[..., None, None]
    v_here = jnp.where(keep, v_here, jnp.zeros_like(v_here))

    turn = row // n_col
    v_got = []
    for s in range(turns):
        send = lax.dynamic_index_in_dim(v_here, (turn + s) % turns, 2, keepdims=False)
        send = jnp.stack([send[0, 0], send[1, 0], send[1, 1]])
        pairs = []
        for t in range(turns):
            for c in range(n_col):
                for q in range(n_col):
                    pairs.append(((t * n_col + c) * n_col + q, (((t + s) % turns) * n_col + q) * n_col + c))
        v_got.append(lax.ppermute(send, both, pairs))
    v_got = jnp.stack(v_got)

    def gather_u(part):
        got = lax.all_gather(part, "col", axis=1)
        return got.reshape(n_row * rank, order)

    inv_full = [lax.all_gather(inv_here[a].astype(BF), "col", axis=1, tiled=True) for a in range(slots)]
    u0 = gather_u(u_here[0, 0])
    u_low = gather_u(u_here[1, 0])
    u1 = gather_u(u_here[1, 1])
    z_here = jnp.stack([
        jnp.dot(rhs_here[a], inv_here[a], precision=lax.Precision.HIGHEST, preferred_element_type=F32)
        for a in range(slots)
    ])
    z = lax.all_gather(z_here, "col", axis=2, tiled=True)

    msg, far = call(
        functools.partial(first_kernel, dims),
        [
            jax.ShapeDtypeStruct((rank, width), BF),
            jax.ShapeDtypeStruct((turns, rank, width + rank), BF),
        ],
        [],
        here, rhs_here[0], inv_full[0], u0, v_got,
    )

    far_got = []
    for s in range(n_row):
        send = lax.dynamic_index_in_dim(far, ((row + s) % n_row) // n_col, 0, keepdims=False)
        pairs = []
        for k in range(n_row):
            for q in range(n_col):
                to = (k + s) % n_row
                pairs.append((k * n_col + q, ((to // n_col) * n_col + q) * n_col + to % n_col))
        far_got.append(lax.ppermute(send, both, pairs))
    far_got = jnp.stack(far_got)

    def spread(m):
        copies = jnp.broadcast_to(m[None], (n_row * n_col,) + m.shape)
        return lax.all_to_all(copies, both, split_axis=0, concat_axis=0, tiled=True)

    q_scratch = [pltpu.VMEM((n_row, width + rank, r_cols), BF)]
    msg, minus, y0 = call(
        functools.partial(middle_kernel, dims),
        [
            jax.ShapeDtypeStruct((rank, width), BF),
            jax.ShapeDtypeStruct((r_cols, order), F32),
            jax.ShapeDtypeStruct((r_cols, order), F32),
        ],
        q_scratch,
        here, spread(msg), far_got, rhs_here[1], inv_full[1], u_low, u1, v_got, z[0], inv_full[0], u0,
    )
    (y1,) = call(
        functools.partial(last_kernel, dims),
        [jax.ShapeDtypeStruct((r_cols, order), F32)],
        q_scratch,
        here, spread(msg), minus, inv_full[1], u1, z[1],
    )
    return jnp.stack([y0, y1])[:, None]


def solution(mesh):
    in_specs = (
        P(None, "row", None, None),
        P(None, "row", None, "col"),
        P(None, "row", None, "col", None, None),
        P(None, "row", None, "col", None, None),
        P(None, "row", None, "col"),
    )
    out_specs = P(None, "row", None, None)
    return jax.shard_map(
        on_device, mesh=mesh, in_specs=in_specs, out_specs=out_specs, check_vma=False
    )
```

```python
import functools

import jax
import jax.numpy as jnp
from jax import lax
from jax.experimental import pallas as pl
from jax.experimental.pallas import tpu as pltpu
from jax.sharding import PartitionSpec as P

BF = jnp.bfloat16
F32 = jnp.float32
NT = (((1,), (1,)), ((), ()))
TN = (((0,), (0,)), ((), ()))
TURNS = 2


def mm(a, b):
    return jnp.dot(a, b, preferred_element_type=F32)


def split_mm(a, b):
    high = a.astype(BF)
    low = (a - high.astype(F32)).astype(BF)
    return mm(high, b) + mm(low, b)


def pack(low, high, both, half):
    return jnp.concatenate([high[:, :half], jnp.where(both, low[:, :half], high[:, half:])], axis=1)


def place(n_col):
    return lax.axis_index("row"), lax.axis_index("col"), lax.axis_index("row") // n_col


def put_columns(out_ref, at, rows, block):
    lanes = out_ref.shape[1]
    count = block.shape[1] // lanes
    for m in range(count):
        out_ref[at + m * rows : at + (m + 1) * rows, :] = block[:, m * lanes : (m + 1) * lanes]


def columns(ref, source, at, rows, start, stop, count):
    return jnp.concatenate([ref[source, at + m * rows + start : at + m * rows + stop, :] for m in range(count)], axis=1)


def prep_kernel(dims, ranks_ref, inv_ref, u_ref, v_ref, send_ref, near_ref):
    n_row, n_col, r_cols, rank, width, half = dims
    row, col, turn = place(n_col)
    order = inv_ref.shape[1]
    near_ref[:order, :] = inv_ref[0].astype(BF)
    put_columns(near_ref, order, TURNS * rank, u_ref[0, 0].reshape(TURNS * rank, order))
    rank_rows = lax.broadcasted_iota(jnp.int32, v_ref.shape[3:], 0)
    for s in range(TURNS):
        t = lax.rem(turn + s, TURNS)
        for n, (i, k) in enumerate(((0, 0), (1, 0), (1, 1))):
            keep = rank_rows < ranks_ref[(i * 2 + k) * TURNS + t]
            v = v_ref[i, k, t]
            send_ref[s, n] = jnp.where(keep, v, jnp.zeros_like(v))


def gathered_inverse(ref, order):
    return jnp.concatenate([ref[c, :order, :] for c in range(ref.shape[0])], axis=1)


def gathered_u(ref, at, rank, blocks):
    n_col = ref.shape[0]
    return jnp.concatenate(
        [columns(ref, j % n_col, at, TURNS * rank, (j // n_col) * rank, (j // n_col + 1) * rank, n_col)
         for j in range(blocks)], axis=0)


def first_kernel(dims, rhs_ref, near_ref, v_a_ref, v_b_ref, msg_ref, far_ref):
    n_row, n_col, r_cols, rank, width, half = dims
    row, col, turn = place(n_col)
    order = rhs_ref.shape[2]
    inv = gathered_inverse(near_ref, order)
    z = split_mm(rhs_ref[0], inv)
    w = mm(gathered_u(near_ref, order, rank, n_row - 1), inv)
    x = jnp.concatenate([z.astype(BF), w.astype(BF)], axis=0)
    near = []
    for t in range(TURNS):
        straight = turn == t
        v = jnp.where(straight, v_a_ref[:2], v_b_ref[:2]).reshape(2 * rank, order)
        tile = lax.dot_general(v, x, NT, preferred_element_type=F32).astype(BF)
        near.append(tile[:rank, :width])
        to = lax.rem(turn + t, TURNS)
        far_ref[lax.rem(TURNS + t - turn, TURNS)] = tile[rank:]
    msg = pack(near[0], near[1], col > row, half)
    for d in range(msg_ref.shape[0]):
        msg_ref[d] = msg


def start_solve(q_ref, n_row, r_cols):
    q_ref[...] = jnp.zeros(q_ref.shape, BF)
    eye = (
        lax.broadcasted_iota(jnp.int32, (r_cols, r_cols), 0)
        == lax.broadcasted_iota(jnp.int32, (r_cols, r_cols), 1)
    ).astype(BF)
    for k in range(n_row):
        q_ref[k, :r_cols, :] = eye


def solve(dims, g_ref, q_ref, extra):
    n_row, n_col, r_cols, rank, width, half = dims
    start_solve(q_ref, n_row, r_cols)
    extras = []
    for k in range(n_row):
        parts = []
        w = half if k <= n_col - 2 else width
        for i in range(k + 1, n_row):
            c, t = i % n_col, i // n_col
            at = half if t == 0 else 0
            parts.append(g_ref[k * n_col + c, :, at : at + w])
        if extra is not None:
            if k == n_row - 1:
                w = width + rank
            parts.append(extra(k)[:, :w])
        if not parts:
            break
        a = parts[0] if len(parts) == 1 else jnp.concatenate(parts, axis=0)
        new = mm(a, q_ref[k, :w, :])
        for i in range(k + 1, n_row):
            at = (i - k - 1) * rank
            q_ref[i, r_cols + k * rank : r_cols + (k + 1) * rank, :] = (-new[at : at + rank]).astype(BF)
        if extra is not None:
            extras.append(new[(n_row - 1 - k) * rank :].astype(BF))
    return extras


def middle_kernel(dims, g_ref, far_ref, rhs_ref, next_ref, u_ref, v_a_ref, v_b_ref, msg_ref, minus_ref, own_ref, q_ref):
    n_row, n_col, r_cols, rank, width, half = dims
    row, col, turn = place(n_col)
    order = rhs_ref.shape[2]
    inv = gathered_inverse(next_ref, order)
    u = jnp.concatenate([u_ref[j % n_col, j // n_col] for j in range(n_row - 2)], axis=0)
    w = mm(u, inv)
    p = solve(dims, g_ref, q_ref, lambda k: far_ref[k % n_col, lax.rem(turn - k // n_col + TURNS, TURNS)])
    total = lax.dot_general(jnp.concatenate(p, axis=0), gathered_u(next_ref, order, rank, n_row), TN,
                            preferred_element_type=F32)
    z = split_mm(rhs_ref[1] - total, inv)
    minus_ref[...] = -total
    x = jnp.concatenate([z.astype(BF), w.astype(BF)], axis=0)
    near = []
    for t in range(TURNS):
        v = jnp.where(turn == t, v_a_ref[2], v_b_ref[2])
        near.append(lax.dot_general(v, x, NT, preferred_element_type=F32).astype(BF))
    msg = pack(near[0], near[1], col > row, half)
    for d in range(msg_ref.shape[0]):
        msg_ref[d] = msg
    own_ref[...] = q_ref[row][r_cols:, :]


def early_kernel(dims, own_ref, near_ref, z_ref, y_ref):
    n_row, n_col, r_cols, rank, width, half = dims
    order = y_ref.shape[1]
    minus = lax.dot_general(own_ref[...], gathered_u(near_ref, order, rank, n_row - 1), TN, preferred_element_type=F32)
    z = jnp.concatenate([z_ref[c, 0] for c in range(n_col)], axis=1)
    y_ref[...] = z + split_mm(minus, gathered_inverse(near_ref, order))


def last_kernel(dims, g_ref, minus_ref, next_ref, u_ref, z_ref, early_ref, y_ref, q_ref):
    n_row, n_col, r_cols, rank, width, half = dims
    order = minus_ref.shape[1]
    y_ref[0] = early_ref[...]
    solve(dims, g_ref, q_ref, None)
    own = q_ref[lax.axis_index("row")][r_cols:, :]
    u = jnp.concatenate([u_ref[j % n_col, j // n_col] for j in range(n_row - 1)], axis=0)
    minus = minus_ref[...] + lax.dot_general(own, u, TN, preferred_element_type=F32)
    z = jnp.concatenate([z_ref[c, 1] for c in range(n_col)], axis=1)
    y_ref[1] = z + split_mm(minus, gathered_inverse(next_ref, order))


def call(kernel, outs, *args, scratch=(), scalars=0, name=None):
    vmem = pl.BlockSpec(memory_space=pltpu.VMEM)
    return pl.pallas_call(
        kernel,
        out_shape=outs,
        in_specs=[pl.BlockSpec(memory_space=pltpu.SMEM)] * scalars + [vmem] * (len(args) - scalars),
        out_specs=[vmem] * len(outs),
        scratch_shapes=list(scratch),
        name=name,
    )(*args)


def on_device(rhs, inverse_t, u_factors, v_factors, tile_ranks):
    slots, _, r_cols, order = rhs.shape
    rank = u_factors.shape[4]
    n_row = lax.axis_size("row")
    n_col = lax.axis_size("col")
    assert slots == 2 and n_row == TURNS * n_col and u_factors.shape[2] == slots * TURNS
    both = ("row", "col")
    lanes = order // n_col
    width = r_cols + (n_row - 2) * rank
    half = r_cols + (n_col - 2) * rank
    assert 2 * half == width
    dims = (n_row, n_col, r_cols, rank, width, half)
    shape = jax.ShapeDtypeStruct
    devices = n_row * n_col

    rhs_here = rhs[:, 0]
    inv_here = inverse_t[:, 0]
    u_here = u_factors[:, 0, :, 0].reshape(slots, slots, TURNS, rank, order)
    v_here = v_factors[:, 0, :, 0].reshape(slots, slots, TURNS, rank, order)
    ranks = tile_ranks.reshape(-1)

    def turn_rows(parts):
        got = []
        for s in range(TURNS):
            pairs = []
            for t in range(TURNS):
                for c in range(n_col):
                    for q in range(n_col):
                        pairs.append(((t * n_col + c) * n_col + q, (((t + s) % TURNS) * n_col + q) * n_col + c))
            got.append(lax.ppermute(parts[s], both, pairs))
        return got

    def spread(m):
        return lax.all_to_all(m, both, split_axis=0, concat_axis=0, tiled=True)

    def kernel(body):
        return functools.partial(body, dims)

    u_rows = n_col * TURNS * rank
    v_send, near = call(
        kernel(prep_kernel),
        [shape((TURNS, 3, rank, order), BF), shape((order + u_rows, lanes), BF)],
        ranks, inv_here, u_here, v_here, scalars=1, name="prep",
    )
    v_a, v_b = turn_rows(v_send)
    near = lax.all_gather(near, "col")

    msg, far = call(
        kernel(first_kernel),
        [shape((devices, rank, width), BF), shape((TURNS, rank, width + rank), BF)],
        rhs_here, near, v_a, v_b, name="first",
    )

    later_inv, later_u_low, later_u, msg, far = lax.optimization_barrier(
        (inv_here[1], u_here[1, 0], u_here[1, 1], msg, far))
    got = spread(msg)
    far = lax.all_gather(jnp.stack(turn_rows(far)), "col")
    nxt = jnp.concatenate([later_inv.astype(BF)] + [
        later_u_low.reshape(TURNS * rank, order)[:, m * lanes : (m + 1) * lanes] for m in range(n_col)], axis=0)
    nxt = lax.all_gather(nxt, "col")
    u_next = lax.all_gather(later_u, "col")

    q_scratch = [pltpu.VMEM((n_row, width + rank, r_cols), BF)]
    msg, minus, own = call(
        kernel(middle_kernel),
        [shape((devices, rank, width), BF), shape((r_cols, order), F32), shape((width + rank - r_cols, r_cols), BF)],
        got, far, rhs_here, nxt, u_next, v_a, v_b, scratch=q_scratch, name="middle",
    )
    rhs_late, inv_late, msg = lax.optimization_barrier((rhs_here, inv_here, msg))
    got = spread(msg)
    z = lax.dot_general(rhs_late, inv_late, (((2,), (1,)), ((0,), (0,))), precision=lax.Precision.HIGHEST,
                        preferred_element_type=F32)
    z = lax.all_gather(z, "col")
    (early,) = call(kernel(early_kernel), [shape((r_cols, order), F32)], own, near, z, name="early")
    (y,) = call(
        kernel(last_kernel), [shape((slots, r_cols, order), F32)],
        got, minus, nxt, u_next, z, early, scratch=q_scratch, name="last",
    )
    return y[:, None]


def solution(mesh):
    in_specs = (
        P(None, "row", None, None),
        P(None, "row", None, "col"),
        P(None, "row", None, "col", None, None),
        P(None, "row", None, "col", None, None),
        P(None, "row", None, "col"),
    )
    out_specs = P(None, "row", None, None)
    return jax.shard_map(
        on_device, mesh=mesh, in_specs=in_specs, out_specs=out_specs, check_vma=False
    )
```

```python
import functools

import jax
import jax.numpy as jnp
from jax import lax
from jax.experimental import pallas as pl
from jax.experimental.pallas import tpu as pltpu
from jax.sharding import Mesh
from jax.sharding import PartitionSpec as P

BF = jnp.bfloat16
F32 = jnp.float32
NT = (((1,), (1,)), ((), ()))
TN = (((0,), (0,)), ((), ()))
TURNS = 2


def mm(a, b):
    return jnp.dot(a, b, preferred_element_type=F32)


def split_mm(a, b):
    high = a.astype(BF)
    low = (a - high.astype(F32)).astype(BF)
    return mm(high, b) + mm(low, b)


def pack(low, high, both, half):
    return jnp.concatenate([high[:, :half], jnp.where(both, low[:, :half], high[:, half:])], axis=1)


def place():
    row, x, core = lax.axis_index("row"), lax.axis_index("x"), lax.axis_index("core")
    n_col = lax.axis_size("x") * lax.axis_size("core")
    return row, x * lax.axis_size("core") + core, row // n_col


def join(scratch, pieces):
    x, core, n_x = lax.axis_index("x"), lax.axis_index("core"), lax.axis_size("x")
    for s in range(n_x):
        for other in range(2):
            source = lax.rem(x - s + n_x, n_x) * 2 + (1 - core if other else core)
            scratch[source] = pieces[2 * s + other][...]


def put_columns(out_ref, at, rows, block):
    lanes = out_ref.shape[1]
    count = block.shape[1] // lanes
    for m in range(count):
        out_ref[at + m * rows : at + (m + 1) * rows, :] = block[:, m * lanes : (m + 1) * lanes]


def columns(ref, source, at, rows, start, stop, count):
    return jnp.concatenate([ref[source, at + m * rows + start : at + m * rows + stop, :] for m in range(count)], axis=1)


def prep_kernel(dims, ranks_ref, inv_ref, u_ref, v_ref, send_a_ref, send_b_ref, near_ref):
    n_row, n_col, r_cols, rank, width, half = dims
    row, col, turn = place()
    order = inv_ref.shape[1]
    near_ref[:order, :] = inv_ref[0].astype(BF)
    put_columns(near_ref, order, TURNS * rank, u_ref[0, 0].reshape(TURNS * rank, order))
    rank_rows = lax.broadcasted_iota(jnp.int32, v_ref.shape[3:], 0)
    for s, send_ref in enumerate((send_a_ref, send_b_ref)):
        t = lax.rem(turn + s, TURNS)
        for n, (i, k) in enumerate(((0, 0), (1, 0), (1, 1))):
            keep = rank_rows < ranks_ref[i, 0, 0, k * TURNS + t]
            v = v_ref[i, k, t]
            send_ref[n] = jnp.where(keep, v, jnp.zeros_like(v))


def gathered_inverse(ref, order):
    return jnp.concatenate([ref[c, :order, :] for c in range(ref.shape[0])], axis=1)


def gathered_u(ref, at, rank, blocks):
    n_col = ref.shape[0]
    return jnp.concatenate(
        [columns(ref, j % n_col, at, TURNS * rank, (j // n_col) * rank, (j // n_col + 1) * rank, n_col)
         for j in range(blocks)], axis=0)


def first_kernel(dims, *refs):
    n_row, n_col, r_cols, rank, width, half = dims
    rhs_ref, v_a_ref, v_b_ref = refs[:3]
    msg_ref, far_a_ref, far_b_ref, near_ref = refs[-4:]
    row, col, turn = place()
    order = rhs_ref.shape[2]
    join(near_ref, refs[3:-4])
    inv = gathered_inverse(near_ref, order)
    z = split_mm(rhs_ref[0], inv)
    w = mm(gathered_u(near_ref, order, rank, n_row - 1), inv)
    x = jnp.concatenate([z.astype(BF), w.astype(BF)], axis=0)
    tiles = []
    for v_ref in (v_a_ref, v_b_ref):
        v = v_ref[:2].reshape(2 * rank, order)
        tiles.append(lax.dot_general(v, x, NT, preferred_element_type=F32).astype(BF))
    straight = turn == 0
    low = jnp.where(straight, tiles[0][:rank, :width], tiles[1][:rank, :width])
    high = jnp.where(straight, tiles[1][:rank, :width], tiles[0][:rank, :width])
    far_a_ref[...] = tiles[0][rank:]
    far_b_ref[...] = tiles[1][rank:]
    msg = pack(low, high, col > row, half)
    for d in range(msg_ref.shape[0]):
        msg_ref[d] = msg


def start_solve(q_ref, n_row, r_cols):
    q_ref[...] = jnp.zeros(q_ref.shape, BF)
    eye = (
        lax.broadcasted_iota(jnp.int32, (r_cols, r_cols), 0)
        == lax.broadcasted_iota(jnp.int32, (r_cols, r_cols), 1)
    ).astype(BF)
    for k in range(n_row):
        q_ref[k, :r_cols, :] = eye


def solve(dims, same_ref, other_ref, g_ref, q_ref, extra):
    n_row, n_col, r_cols, rank, width, half = dims
    core = lax.axis_index("core")
    g_ref[core] = same_ref[...]
    g_ref[1 - core] = other_ref[...]
    start_solve(q_ref, n_row, r_cols)
    extras = []
    for k in range(n_row):
        parts = []
        w = half if k <= n_col - 2 else width
        for i in range(k + 1, n_row):
            c, t = i % n_col, i // n_col
            at = half if t == 0 else 0
            parts.append(g_ref[c % 2, k * (n_col // 2) + c // 2, :, at : at + w])
        if extra is not None:
            if k == n_row - 1:
                w = width + rank
            parts.append(extra(k)[:, :w])
        if not parts:
            break
        a = parts[0] if len(parts) == 1 else jnp.concatenate(parts, axis=0)
        new = mm(a, q_ref[k, :w, :])
        for i in range(k + 1, n_row):
            at = (i - k - 1) * rank
            q_ref[i, r_cols + k * rank : r_cols + (k + 1) * rank, :] = (-new[at : at + rank]).astype(BF)
        if extra is not None:
            extras.append(new[(n_row - 1 - k) * rank :].astype(BF))
    return extras


def middle_kernel(dims, *refs):
    n_row, n_col, r_cols, rank, width, half = dims
    same_ref, other_ref, rhs_ref, v_a_ref, v_b_ref = refs[:5]
    fars, nexts = refs[5 : 5 + n_col], refs[5 + n_col : 5 + 2 * n_col]
    msg_ref, minus_ref, own_ref, g_ref, q_ref, far_ref, next_ref = refs[5 + 2 * n_col :]
    row, col, turn = place()
    order = rhs_ref.shape[2]
    rows = n_col * TURNS * rank
    join(next_ref, nexts)
    join(far_ref, fars)
    inv = gathered_inverse(next_ref, order)
    w = mm(gathered_u(next_ref, order + rows, rank, n_row - 2), inv)
    p = solve(dims, same_ref, other_ref, g_ref, q_ref,
              lambda k: far_ref[k % n_col, lax.rem(turn - k // n_col + TURNS, TURNS)])
    total = lax.dot_general(jnp.concatenate(p, axis=0), gathered_u(next_ref, order, rank, n_row), TN,
                            preferred_element_type=F32)
    z = split_mm(rhs_ref[1] - total, inv)
    minus_ref[...] = -total
    x = jnp.concatenate([z.astype(BF), w.astype(BF)], axis=0)
    tiles = [lax.dot_general(v_ref[2], x, NT, preferred_element_type=F32).astype(BF) for v_ref in (v_a_ref, v_b_ref)]
    straight = turn == 0
    low = jnp.where(straight, tiles[0], tiles[1])
    high = jnp.where(straight, tiles[1], tiles[0])
    msg = pack(low, high, col > row, half)
    for d in range(msg_ref.shape[0]):
        msg_ref[d] = msg
    own_ref[...] = q_ref[row][r_cols:, :]


def early_kernel(dims, *refs):
    n_row, n_col, r_cols, rank, width, half = dims
    own_ref = refs[0]
    nears, zs = refs[1 : 1 + n_col], refs[1 + n_col : 1 + 2 * n_col]
    y_ref, z_out_ref, near_ref, z_ref = refs[1 + 2 * n_col :]
    order = y_ref.shape[1]
    join(near_ref, nears)
    join(z_ref, zs)
    minus = lax.dot_general(own_ref[...], gathered_u(near_ref, order, rank, n_row - 1), TN, preferred_element_type=F32)
    z = jnp.concatenate([z_ref[c, 0] for c in range(n_col)], axis=1)
    y_ref[...] = z + split_mm(minus, gathered_inverse(near_ref, order))
    z_out_ref[...] = jnp.concatenate([z_ref[c, 1] for c in range(n_col)], axis=1)


def last_kernel(dims, *refs):
    n_row, n_col, r_cols, rank, width, half = dims
    same_ref, other_ref, minus_ref, z_ref, early_ref = refs[:5]
    y_ref, g_ref, q_ref, next_ref = refs[5 + n_col :]
    order = minus_ref.shape[1]
    y_ref[0] = early_ref[...]
    join(next_ref, refs[5 : 5 + n_col])
    solve(dims, same_ref, other_ref, g_ref, q_ref, None)
    own = q_ref[lax.axis_index("row")][r_cols:, :]
    u = gathered_u(next_ref, order + n_col * TURNS * rank, rank, n_row - 1)
    minus = minus_ref[...] + lax.dot_general(own, u, TN, preferred_element_type=F32)
    y_ref[1] = z_ref[...] + split_mm(minus, gathered_inverse(next_ref, order))


def call(kernel, outs, *args, scratch=(), scalars=0, name=None):
    vmem = pl.BlockSpec(memory_space=pltpu.VMEM)
    return pl.pallas_call(
        kernel,
        out_shape=outs,
        in_specs=[pl.BlockSpec(memory_space=pltpu.SMEM)] * scalars + [vmem] * (len(args) - scalars),
        out_specs=[vmem] * len(outs),
        scratch_shapes=list(scratch),
        compiler_params=pltpu.CompilerParams(vmem_limit_bytes=VMEM_LIMIT),
        name=name,
    )(*args)


VMEM_LIMIT = 24 * 2**20


def on_device(rhs, inverse_t, u_factors, v_factors, tile_ranks):
    slots, _, r_cols, order = rhs.shape
    rank = u_factors.shape[4]
    n_row = lax.axis_size("row")
    n_x = lax.axis_size("x")
    n_col = 2 * n_x
    assert slots == 2 and n_row == TURNS * n_col and u_factors.shape[2] == slots * TURNS
    everywhere = ("row", "x", "core")
    lanes = order // n_col
    width = r_cols + (n_row - 2) * rank
    half = r_cols + (n_col - 2) * rank
    assert 2 * half == width
    dims = (n_row, n_col, r_cols, rank, width, half)
    shape = jax.ShapeDtypeStruct
    swap = [(0, 1), (1, 0)]

    rhs_here = rhs[:, 0]
    inv_here = inverse_t[:, 0]
    u_here = u_factors[:, 0, :, 0].reshape(slots, slots, TURNS, rank, order)
    v_here = v_factors[:, 0, :, 0].reshape(slots, slots, TURNS, rank, order)
    ranks = jnp.swapaxes(tile_ranks, 2, 3)

    def gather(part):
        pieces = []
        for s in range(n_x):
            moved = lax.ppermute(part, "x", [(i, (i + s) % n_x) for i in range(n_x)]) if s else part
            pieces += [moved, lax.ppermute(moved, "core", swap)]
        return pieces

    def turn_rows(parts):
        got = []
        for s in range(TURNS):
            pairs = []
            for t in range(TURNS):
                for c in range(n_col):
                    for q in range(n_col):
                        pairs.append(((t * n_col + c) * n_col + q, (((t + s) % TURNS) * n_col + q) * n_col + c))
            got.append(lax.ppermute(parts[s], everywhere, pairs))
        return got

    def spread(m):
        same = lax.all_to_all(m, ("row", "x"), split_axis=0, concat_axis=0, tiled=True)
        return same, lax.ppermute(same, "core", swap)

    def kernel(body):
        return functools.partial(body, dims)

    u_rows = n_col * TURNS * rank
    messages = shape((n_row * n_x, rank, width), BF)
    far_shape = shape((rank, width + rank), BF)
    near_scratch = pltpu.VMEM((n_col, order + u_rows, lanes), BF)
    next_scratch = pltpu.VMEM((n_col, order + 2 * u_rows, lanes), BF)
    solve_scratch = [
        pltpu.VMEM((2, n_row * n_x, rank, width), BF),
        pltpu.VMEM((n_row, width + rank, r_cols), BF),
    ]

    v_send = shape((3, rank, order), BF)
    v_a, v_b, near = call(
        kernel(prep_kernel),
        [v_send, v_send, shape((order + u_rows, lanes), BF)],
        ranks, inv_here, u_here, v_here, scalars=1, name="prep",
    )
    near = gather(near)
    v_a, v_b = turn_rows([v_a, v_b])

    msg, far_a, far_b = call(
        kernel(first_kernel), [messages, far_shape, far_shape],
        rhs_here, v_a, v_b, *near, scratch=[near_scratch], name="first",
    )

    later_inv, later_u, msg, far_a, far_b = lax.optimization_barrier(
        (inv_here[1], u_here[1], msg, far_a, far_b))
    same, other = spread(msg)
    far = gather(jnp.stack(turn_rows([far_a, far_b])))
    later_u = later_u.reshape(slots, TURNS * rank, order)
    nxt = gather(jnp.concatenate([later_inv.astype(BF)] + [
        later_u[a, :, m * lanes : (m + 1) * lanes] for a in range(slots) for m in range(n_col)], axis=0))

    msg, minus, own = call(
        kernel(middle_kernel),
        [messages, shape((r_cols, order), F32), shape((width + rank - r_cols, r_cols), BF)],
        same, other, rhs_here, v_a, v_b, *far, *nxt,
        scratch=solve_scratch + [pltpu.VMEM((n_col, TURNS, rank, width + rank), BF), next_scratch], name="middle",
    )
    rhs_late, inv_late, msg = lax.optimization_barrier((rhs_here, inv_here, msg))
    same, other = spread(msg)
    z = gather(lax.dot_general(rhs_late, inv_late, (((2,), (1,)), ((0,), (0,))), precision=lax.Precision.HIGHEST,
                               preferred_element_type=F32))
    early, z_last = call(
        kernel(early_kernel), [shape((r_cols, order), F32)] * 2, own, *near, *z,
        scratch=[near_scratch, pltpu.VMEM((n_col, slots, r_cols, lanes), F32)], name="early")
    (y,) = call(
        kernel(last_kernel), [shape((slots, r_cols, order), F32)],
        same, other, minus, z_last, early, *nxt, scratch=solve_scratch + [next_scratch], name="last",
    )
    return y[:, None]


def solution(mesh):
    n_row, n_col = (mesh.shape[name] for name in ("row", "col"))
    fine = Mesh(mesh.devices.reshape(n_row, n_col // 2, 2), ("row", "x", "core"))
    col = ("x", "core")
    in_specs = (
        P(None, "row", None, None),
        P(None, "row", None, col),
        P(None, "row", None, col, None, None),
        P(None, "row", None, col, None, None),
        P(None, "row", None, col),
    )
    out_specs = P(None, "row", None, None)
    return jax.shard_map(
        on_device, mesh=fine, in_specs=in_specs, out_specs=out_specs, check_vma=False
    )
```

```python
import functools

import jax
import jax.numpy as jnp
from jax import lax
from jax.experimental import pallas as pl
from jax.experimental.pallas import tpu as pltpu
from jax.sharding import Mesh
from jax.sharding import PartitionSpec as P

BF = jnp.bfloat16
F32 = jnp.float32
NT = (((1,), (1,)), ((), ()))
TN = (((0,), (0,)), ((), ()))
TURNS = 2


def mm(a, b):
    return jnp.dot(a, b, preferred_element_type=F32)


def split_mm(a, b):
    high = a.astype(BF)
    low = (a - high.astype(F32)).astype(BF)
    return mm(high, b) + mm(low, b)


def pack(low, high, both, half):
    return jnp.concatenate([high[:, :half], jnp.where(both, low[:, :half], high[:, half:])], axis=1)


def place():
    row, x, core = lax.axis_index("row"), lax.axis_index("x"), lax.axis_index("core")
    n_col = lax.axis_size("x") * lax.axis_size("core")
    return row, x * lax.axis_size("core") + core, row // n_col


def join(scratch, pieces):
    x, core, n_x = lax.axis_index("x"), lax.axis_index("core"), lax.axis_size("x")
    for s in range(n_x):
        for other in range(2):
            source = lax.rem(x - s + n_x, n_x) * 2 + (1 - core if other else core)
            scratch[source] = pieces[2 * s + other][...]


def put_columns(out_ref, at, rows, block):
    lanes = out_ref.shape[1]
    count = block.shape[1] // lanes
    for m in range(count):
        out_ref[at + m * rows : at + (m + 1) * rows, :] = block[:, m * lanes : (m + 1) * lanes]


def columns(ref, source, at, rows, start, stop, count):
    return jnp.concatenate([ref[source, at + m * rows + start : at + m * rows + stop, :] for m in range(count)], axis=1)


def prep_kernel(dims, ranks_ref, inv_hbm, u_hbm, v_hbm, send_a_ref, send_b_ref, near_ref, inv_ref, u_ref, v_ref, sems):
    _, _, _, rank, _, _ = dims
    _, _, turn = place()
    order = inv_ref.shape[0]
    copies = [
        pltpu.make_async_copy(inv_hbm.at[0], inv_ref, sems.at[0]),
        pltpu.make_async_copy(u_hbm.at[0, 0], u_ref, sems.at[1]),
        pltpu.make_async_copy(v_hbm, v_ref, sems.at[2]),
    ]
    for copy in copies:
        copy.start()
    copies[0].wait()
    copies[1].wait()
    near_ref[:order, :] = inv_ref[...].astype(BF)
    put_columns(near_ref, order, TURNS * rank, u_ref[...].reshape(TURNS * rank, order))
    copies[2].wait()
    rank_rows = lax.broadcasted_iota(jnp.int32, v_ref.shape[3:], 0)
    for s, send_ref in enumerate((send_a_ref, send_b_ref)):
        t = lax.rem(turn + s, TURNS)
        for n, (i, k) in enumerate(((0, 0), (1, 0), (1, 1))):
            keep = rank_rows < ranks_ref[i, 0, 0, k * TURNS + t]
            v = v_ref[i, k, t]
            send_ref[n] = jnp.where(keep, v, jnp.zeros_like(v))


def gathered_inverse(ref, order):
    return jnp.concatenate([ref[c, :order, :] for c in range(ref.shape[0])], axis=1)


def gathered_u(ref, at, rank, blocks):
    n_col = ref.shape[0]
    return jnp.concatenate(
        [columns(ref, j % n_col, at, TURNS * rank, (j // n_col) * rank, (j // n_col + 1) * rank, n_col)
         for j in range(blocks)], axis=0)


def first_kernel(dims, *refs):
    n_row, _, _, rank, width, half = dims
    rhs_ref, v_a_ref, v_b_ref = refs[:3]
    msg_ref, far_a_ref, far_b_ref, near_ref = refs[-4:]
    row, col, turn = place()
    order = rhs_ref.shape[2]
    join(near_ref, refs[3:-4])
    inv = gathered_inverse(near_ref, order)
    z = split_mm(rhs_ref[0], inv)
    w = mm(gathered_u(near_ref, order, rank, n_row - 1), inv)
    x = jnp.concatenate([z.astype(BF), w.astype(BF)], axis=0)
    tiles = []
    for v_ref in (v_a_ref, v_b_ref):
        v = v_ref[:2].reshape(2 * rank, order)
        tiles.append(lax.dot_general(v, x, NT, preferred_element_type=F32).astype(BF))
    straight = turn == 0
    low = jnp.where(straight, tiles[0][:rank, :width], tiles[1][:rank, :width])
    high = jnp.where(straight, tiles[1][:rank, :width], tiles[0][:rank, :width])
    far_a_ref[...] = tiles[0][rank:]
    far_b_ref[...] = tiles[1][rank:]
    msg = pack(low, high, col > row, half)
    for d in range(msg_ref.shape[0]):
        msg_ref[d] = msg


def start_solve(q_ref, n_row, r_cols):
    q_ref[...] = jnp.zeros(q_ref.shape, BF)
    eye = (
        lax.broadcasted_iota(jnp.int32, (r_cols, r_cols), 0)
        == lax.broadcasted_iota(jnp.int32, (r_cols, r_cols), 1)
    ).astype(BF)
    for k in range(n_row):
        q_ref[k, :r_cols, :] = eye


def solve(dims, same_ref, other_ref, g_ref, q_ref, extra):
    n_row, n_col, r_cols, rank, width, half = dims
    core = lax.axis_index("core")
    g_ref[core] = same_ref[...]
    g_ref[1 - core] = other_ref[...]
    start_solve(q_ref, n_row, r_cols)
    extras = []
    for k in range(n_row):
        parts = []
        w = half if k <= n_col - 2 else width
        for i in range(k + 1, n_row):
            c, t = i % n_col, i // n_col
            at = half if t == 0 else 0
            parts.append(g_ref[c % 2, k * (n_col // 2) + c // 2, :, at : at + w])
        if extra is not None:
            if k == n_row - 1:
                w = width + rank
            parts.append(extra(k)[:, :w])
        if not parts:
            break
        a = parts[0] if len(parts) == 1 else jnp.concatenate(parts, axis=0)
        new = mm(a, q_ref[k, :w, :])
        for i in range(k + 1, n_row):
            at = (i - k - 1) * rank
            q_ref[i, r_cols + k * rank : r_cols + (k + 1) * rank, :] = (-new[at : at + rank]).astype(BF)
        if extra is not None:
            extras.append(new[(n_row - 1 - k) * rank :].astype(BF))
    return extras


def middle_kernel(dims, *refs):
    n_row, n_col, r_cols, rank, _, half = dims
    same_ref, other_ref, rhs_ref, v_a_ref, v_b_ref = refs[:5]
    fars, nexts = refs[5 : 5 + n_col], refs[5 + n_col : 5 + 2 * n_col]
    msg_ref, minus_ref, own_ref, g_ref, q_ref, far_ref, next_ref = refs[5 + 2 * n_col :]
    row, col, turn = place()
    order = rhs_ref.shape[2]
    rows = n_col * TURNS * rank
    join(next_ref, nexts)
    join(far_ref, fars)
    inv = gathered_inverse(next_ref, order)
    w = mm(gathered_u(next_ref, order + rows, rank, n_row - 2), inv)
    p = solve(dims, same_ref, other_ref, g_ref, q_ref,
              lambda k: far_ref[k % n_col, lax.rem(turn - k // n_col + TURNS, TURNS)])
    total = lax.dot_general(jnp.concatenate(p, axis=0), gathered_u(next_ref, order, rank, n_row), TN,
                            preferred_element_type=F32)
    z = split_mm(rhs_ref[1] - total, inv)
    minus_ref[...] = -total
    x = jnp.concatenate([z.astype(BF), w.astype(BF)], axis=0)
    tiles = [lax.dot_general(v_ref[2], x, NT, preferred_element_type=F32).astype(BF) for v_ref in (v_a_ref, v_b_ref)]
    straight = turn == 0
    low = jnp.where(straight, tiles[0], tiles[1])
    high = jnp.where(straight, tiles[1], tiles[0])
    msg = pack(low, high, col > row, half)
    for d in range(msg_ref.shape[0]):
        msg_ref[d] = msg
    own_ref[...] = q_ref[row][r_cols:, :]


def early_kernel(dims, *refs):
    n_row, n_col, _, rank, _, _ = dims
    own_ref = refs[0]
    nears, zs = refs[1 : 1 + n_col], refs[1 + n_col : 1 + 2 * n_col]
    y_ref, z_out_ref, near_ref, z_ref = refs[1 + 2 * n_col :]
    order = y_ref.shape[1]
    join(near_ref, nears)
    join(z_ref, zs)
    minus = lax.dot_general(own_ref[...], gathered_u(near_ref, order, rank, n_row - 1), TN, preferred_element_type=F32)
    z = jnp.concatenate([z_ref[c, 0] for c in range(n_col)], axis=1)
    y_ref[...] = z + split_mm(minus, gathered_inverse(near_ref, order))
    z_out_ref[...] = jnp.concatenate([z_ref[c, 1] for c in range(n_col)], axis=1)


def last_kernel(dims, *refs):
    n_row, n_col, r_cols, rank, _, _ = dims
    same_ref, other_ref, minus_ref, z_ref, early_ref = refs[:5]
    y_ref, g_ref, q_ref, next_ref = refs[5 + n_col :]
    order = minus_ref.shape[1]
    y_ref[0] = early_ref[...]
    join(next_ref, refs[5 : 5 + n_col])
    solve(dims, same_ref, other_ref, g_ref, q_ref, None)
    own = q_ref[lax.axis_index("row")][r_cols:, :]
    u = gathered_u(next_ref, order + n_col * TURNS * rank, rank, n_row - 1)
    minus = minus_ref[...] + lax.dot_general(own, u, TN, preferred_element_type=F32)
    y_ref[1] = z_ref[...] + split_mm(minus, gathered_inverse(next_ref, order))


def call(kernel, outs, *args, scratch=(), scalars=0, far=False, limit=24 * 2**20):
    vmem = pl.BlockSpec(memory_space=pltpu.VMEM)
    place_in = pl.BlockSpec(memory_space=pltpu.HBM) if far else vmem
    return pl.pallas_call(
        kernel,
        out_shape=outs,
        in_specs=[pl.BlockSpec(memory_space=pltpu.SMEM)] * scalars + [place_in] * (len(args) - scalars),
        out_specs=[vmem] * len(outs),
        scratch_shapes=list(scratch),
        compiler_params=pltpu.CompilerParams(vmem_limit_bytes=limit),
    )(*args)


def on_device(rhs, inverse_t, u_factors, v_factors, tile_ranks):
    slots, _, r_cols, order = rhs.shape
    rank = u_factors.shape[4]
    n_row = lax.axis_size("row")
    n_x = lax.axis_size("x")
    n_col = 2 * n_x
    assert slots == 2 and n_row == TURNS * n_col and u_factors.shape[2] == slots * TURNS
    everywhere = ("row", "x", "core")
    lanes = order // n_col
    width = r_cols + (n_row - 2) * rank
    half = r_cols + (n_col - 2) * rank
    assert 2 * half == width
    dims = (n_row, n_col, r_cols, rank, width, half)
    shape = jax.ShapeDtypeStruct
    swap = [(0, 1), (1, 0)]

    rhs_here = rhs[:, 0]
    inv_here = inverse_t[:, 0]
    u_here = u_factors[:, 0, :, 0].reshape(slots, slots, TURNS, rank, order)
    v_here = v_factors[:, 0, :, 0].reshape(slots, slots, TURNS, rank, order)
    ranks = jnp.swapaxes(tile_ranks, 2, 3)

    def gather(part):
        pieces = []
        for s in range(n_x):
            moved = part
            if s:
                moved = lax.ppermute(part, "x", [(i, (i + s) % n_x) for i in range(n_x)])
            pieces += [moved, lax.ppermute(moved, "core", swap)]
        return pieces

    def turn_rows(parts):
        got = []
        for s in range(TURNS):
            pairs = []
            for t in range(TURNS):
                for c in range(n_col):
                    for q in range(n_col):
                        pairs.append(((t * n_col + c) * n_col + q, (((t + s) % TURNS) * n_col + q) * n_col + c))
            got.append(lax.ppermute(parts[s], everywhere, pairs))
        return got

    def spread(m):
        same = lax.all_to_all(m, ("row", "x"), split_axis=0, concat_axis=0, tiled=True)
        return same, lax.ppermute(same, "core", swap)

    def kernel(body):
        return functools.partial(body, dims)

    u_rows = n_col * TURNS * rank
    messages = shape((n_row * n_x, rank, width), BF)
    far_shape = shape((rank, width + rank), BF)
    near_scratch = pltpu.VMEM((n_col, order + u_rows, lanes), BF)
    next_scratch = pltpu.VMEM((n_col, order + 2 * u_rows, lanes), BF)
    solve_scratch = [
        pltpu.VMEM((2, n_row * n_x, rank, width), BF),
        pltpu.VMEM((n_row, width + rank, r_cols), BF),
    ]

    v_send = shape((3, rank, order), BF)
    v_a, v_b, near = call(
        kernel(prep_kernel),
        [v_send, v_send, shape((order + u_rows, lanes), BF)],
        ranks, inv_here, u_here, v_here, scalars=1, far=True, limit=67043328 - 450 * 1024,
        scratch=[
            pltpu.VMEM((order, lanes), F32),
            pltpu.VMEM((TURNS, rank, order), BF),
            pltpu.VMEM((slots, slots, TURNS, rank, order), BF),
            pltpu.SemaphoreType.DMA((3,)),
        ],
    )
    near = gather(near)
    v_a, v_b = turn_rows([v_a, v_b])
    later_u = u_here[1].reshape(slots, TURNS * rank, order)
    nxt = gather(jnp.concatenate([inv_here[1].astype(BF)] + [
        later_u[a, :, m * lanes : (m + 1) * lanes] for a in range(slots) for m in range(n_col)], axis=0))
    z = gather(lax.dot_general(rhs_here, inv_here, (((2,), (1,)), ((0,), (0,))), precision=lax.Precision.HIGHEST,
                               preferred_element_type=F32))

    msg, far_a, far_b = call(
        kernel(first_kernel), [messages, far_shape, far_shape],
        rhs_here, v_a, v_b, *near, scratch=[near_scratch],
    )

    far = gather(jnp.stack(turn_rows([far_a, far_b])))
    same, other = spread(msg)

    msg, minus, own = call(
        kernel(middle_kernel),
        [messages, shape((r_cols, order), F32), shape((width + rank - r_cols, r_cols), BF)],
        same, other, rhs_here, v_a, v_b, *far, *nxt,
        scratch=solve_scratch + [pltpu.VMEM((n_col, TURNS, rank, width + rank), BF), next_scratch],
    )
    same, other = spread(msg)
    early, z_last = call(
        kernel(early_kernel), [shape((r_cols, order), F32)] * 2, own, *near, *z,
        scratch=[near_scratch, pltpu.VMEM((n_col, slots, r_cols, lanes), F32)])
    (y,) = call(
        kernel(last_kernel), [shape((slots, r_cols, order), F32)],
        same, other, minus, z_last, early, *nxt, scratch=solve_scratch + [next_scratch],
    )
    return y[:, None]


def solution(mesh):
    n_row, n_col = (mesh.shape[name] for name in ("row", "col"))
    fine = Mesh(mesh.devices.reshape(n_row, n_col // 2, 2), ("row", "x", "core"))
    col = ("x", "core")
    in_specs = (
        P(None, "row", None, None),
        P(None, "row", None, col),
        P(None, "row", None, col, None, None),
        P(None, "row", None, col, None, None),
        P(None, "row", None, col),
    )
    out_specs = P(None, "row", None, None)
    return jax.shard_map(on_device, mesh=fine, in_specs=in_specs, out_specs=out_specs, check_vma=False)
```

```python
import functools

import jax
import jax.numpy as jnp
from jax import lax
from jax.experimental import pallas as pl
from jax.experimental.pallas import tpu as pltpu
from jax.sharding import Mesh
from jax.sharding import PartitionSpec as P

BF = jnp.bfloat16
F32 = jnp.float32
NT = (((1,), (1,)), ((), ()))
TN = (((0,), (0,)), ((), ()))
TURNS = 2


def mm(a, b):
    return jnp.dot(a, b, preferred_element_type=F32)


def split_mm(a, b):
    high = a.astype(BF)
    low = (a - high.astype(F32)).astype(BF)
    return mm(high, b) + mm(low, b)


def pack(low, high, both, half):
    return jnp.concatenate([high[:, :half], jnp.where(both, low[:, :half], high[:, half:])], axis=1)


def place():
    row, x, core = lax.axis_index("row"), lax.axis_index("x"), lax.axis_index("core")
    n_col = lax.axis_size("x") * lax.axis_size("core")
    return row, x * lax.axis_size("core") + core, row // n_col


def join(scratch, pieces):
    x, core, n_x = lax.axis_index("x"), lax.axis_index("core"), lax.axis_size("x")
    for s in range(n_x):
        for other in range(2):
            source = lax.rem(x - s + n_x, n_x) * 2 + (1 - core if other else core)
            scratch[source] = pieces[2 * s + other][...]


def put_columns(out_ref, at, rows, block):
    lanes = out_ref.shape[1]
    count = block.shape[1] // lanes
    for m in range(count):
        out_ref[at + m * rows : at + (m + 1) * rows, :] = block[:, m * lanes : (m + 1) * lanes]


def columns(ref, source, at, rows, start, stop, count):
    return jnp.concatenate([ref[source, at + m * rows + start : at + m * rows + stop, :] for m in range(count)], axis=1)


def prep_kernel(dims, ranks_ref, inv_hbm, u_hbm, v_hbm, send_a_ref, send_b_ref, near_ref, inv_ref, u_ref, v_ref, sems):
    _, _, _, rank, _, _ = dims
    _, _, turn = place()
    order = inv_ref.shape[0]
    copies = [
        pltpu.make_async_copy(inv_hbm.at[0], inv_ref, sems.at[0]),
        pltpu.make_async_copy(u_hbm.at[0, 0], u_ref, sems.at[1]),
        pltpu.make_async_copy(v_hbm, v_ref, sems.at[2]),
    ]
    for copy in copies:
        copy.start()
    copies[0].wait()
    copies[1].wait()
    near_ref[:order, :] = inv_ref[...].astype(BF)
    put_columns(near_ref, order, TURNS * rank, u_ref[...].reshape(TURNS * rank, order))
    copies[2].wait()
    rank_rows = lax.broadcasted_iota(jnp.int32, v_ref.shape[3:], 0)
    for s, send_ref in enumerate((send_a_ref, send_b_ref)):
        t = lax.rem(turn + s, TURNS)
        for n, (i, k) in enumerate(((0, 0), (1, 0), (1, 1))):
            keep = rank_rows < ranks_ref[i, 0, 0, k * TURNS + t]
            v = v_ref[i, k, t]
            send_ref[n] = jnp.where(keep, v, jnp.zeros_like(v))


def gathered_inverse(ref, order):
    return jnp.concatenate([ref[c, :order, :] for c in range(ref.shape[0])], axis=1)


def gathered_u(ref, at, rank, blocks):
    n_col = ref.shape[0]
    return jnp.concatenate(
        [columns(ref, j % n_col, at, TURNS * rank, (j // n_col) * rank, (j // n_col + 1) * rank, n_col)
         for j in range(blocks)], axis=0)


def first_kernel(dims, *refs):
    n_row, _, _, rank, width, half = dims
    rhs_ref, v_a_ref, v_b_ref = refs[:3]
    msg_ref, far_a_ref, far_b_ref, near_ref = refs[-4:]
    row, col, turn = place()
    order = rhs_ref.shape[2]
    join(near_ref, refs[3:-4])
    inv = gathered_inverse(near_ref, order)
    z = split_mm(rhs_ref[0], inv)
    w = mm(gathered_u(near_ref, order, rank, n_row - 1), inv)
    x = jnp.concatenate([z.astype(BF), w.astype(BF)], axis=0)
    tiles = []
    for v_ref in (v_a_ref, v_b_ref):
        v = v_ref[:2].reshape(2 * rank, order)
        tiles.append(lax.dot_general(v, x, NT, preferred_element_type=F32).astype(BF))
    straight = turn == 0
    low = jnp.where(straight, tiles[0][:rank, :width], tiles[1][:rank, :width])
    high = jnp.where(straight, tiles[1][:rank, :width], tiles[0][:rank, :width])
    far_a_ref[...] = tiles[0][rank:]
    far_b_ref[...] = tiles[1][rank:]
    msg = pack(low, high, col > row, half)
    for d in range(msg_ref.shape[0]):
        msg_ref[d] = msg


def start_solve(q_ref, n_row, r_cols):
    q_ref[...] = jnp.zeros(q_ref.shape, BF)
    eye = (
        lax.broadcasted_iota(jnp.int32, (r_cols, r_cols), 0)
        == lax.broadcasted_iota(jnp.int32, (r_cols, r_cols), 1)
    ).astype(BF)
    for k in range(n_row):
        q_ref[k, :r_cols, :] = eye


def solve(dims, same_ref, other_ref, g_ref, q_ref, extra):
    n_row, n_col, r_cols, rank, width, half = dims
    core = lax.axis_index("core")
    g_ref[core] = same_ref[...]
    g_ref[1 - core] = other_ref[...]
    start_solve(q_ref, n_row, r_cols)
    extras = []
    for k in range(n_row):
        parts = []
        w = half if k <= n_col - 2 else width
        for i in range(k + 1, n_row):
            c, t = i % n_col, i // n_col
            at = half if t == 0 else 0
            parts.append(g_ref[c % 2, k * (n_col // 2) + c // 2, :, at : at + w])
        if extra is not None:
            if k == n_row - 1:
                w = width + rank
            parts.append(extra(k)[:, :w])
        if not parts:
            break
        a = parts[0] if len(parts) == 1 else jnp.concatenate(parts, axis=0)
        new = mm(a, q_ref[k, :w, :])
        for i in range(k + 1, n_row):
            at = (i - k - 1) * rank
            q_ref[i, r_cols + k * rank : r_cols + (k + 1) * rank, :] = (-new[at : at + rank]).astype(BF)
        if extra is not None:
            extras.append(new[(n_row - 1 - k) * rank :].astype(BF))
    return extras


def middle_kernel(dims, *refs):
    n_row, n_col, r_cols, rank, _, half = dims
    same_ref, other_ref, rhs_ref, v_a_ref, v_b_ref = refs[:5]
    fars, nexts = refs[5 : 5 + n_col], refs[5 + n_col : 5 + 2 * n_col]
    msg_ref, minus_ref, own_ref, g_ref, q_ref, far_ref, next_ref = refs[5 + 2 * n_col :]
    row, col, turn = place()
    order = rhs_ref.shape[2]
    rows = n_col * TURNS * rank
    join(next_ref, nexts)
    join(far_ref, fars)
    inv = gathered_inverse(next_ref, order)
    w = mm(gathered_u(next_ref, order + rows, rank, n_row - 2), inv)
    p = solve(dims, same_ref, other_ref, g_ref, q_ref,
              lambda k: far_ref[k % n_col, lax.rem(turn - k // n_col + TURNS, TURNS)])
    total = lax.dot_general(jnp.concatenate(p, axis=0), gathered_u(next_ref, order, rank, n_row), TN,
                            preferred_element_type=F32)
    z = split_mm(rhs_ref[1] - total, inv)
    minus_ref[...] = -total
    x = jnp.concatenate([z.astype(BF), w.astype(BF)], axis=0)
    tiles = [lax.dot_general(v_ref[2], x, NT, preferred_element_type=F32).astype(BF) for v_ref in (v_a_ref, v_b_ref)]
    straight = turn == 0
    low = jnp.where(straight, tiles[0], tiles[1])
    high = jnp.where(straight, tiles[1], tiles[0])
    msg = pack(low, high, col > row, half)
    for d in range(msg_ref.shape[0]):
        msg_ref[d] = msg
    own_ref[...] = q_ref[row][r_cols:, :]


def gathered_z(ref, at, r_cols):
    parts = [jnp.concatenate([ref[c, start : start + r_cols, :] for c in range(ref.shape[0])], axis=1).astype(F32)
             for start in (at, at + r_cols)]
    return parts[0] + parts[1]


def early_kernel(dims, *refs):
    n_row, n_col, r_cols, rank, _, _ = dims
    own_ref = refs[0]
    nears, nexts = refs[1 : 1 + n_col], refs[1 + n_col : 1 + 2 * n_col]
    y_ref, near_ref, next_ref = refs[1 + 2 * n_col :]
    order = y_ref.shape[1]
    at = order + 2 * n_col * TURNS * rank
    join(near_ref, nears)
    join(next_ref, nexts)
    minus = lax.dot_general(own_ref[...], gathered_u(near_ref, order, rank, n_row - 1), TN, preferred_element_type=F32)
    y_ref[...] = gathered_z(next_ref, at, r_cols) + split_mm(minus, gathered_inverse(near_ref, order))


def last_kernel(dims, *refs):
    n_row, n_col, r_cols, rank, _, _ = dims
    same_ref, other_ref, minus_ref, early_ref = refs[:4]
    y_ref, g_ref, q_ref, next_ref = refs[4 + n_col :]
    order = minus_ref.shape[1]
    rows = n_col * TURNS * rank
    y_ref[0] = early_ref[...]
    join(next_ref, refs[4 : 4 + n_col])
    solve(dims, same_ref, other_ref, g_ref, q_ref, None)
    own = q_ref[lax.axis_index("row")][r_cols:, :]
    u = gathered_u(next_ref, order + rows, rank, n_row - 1)
    minus = minus_ref[...] + lax.dot_general(own, u, TN, preferred_element_type=F32)
    z = gathered_z(next_ref, order + 2 * rows + 2 * r_cols, r_cols)
    y_ref[1] = z + split_mm(minus, gathered_inverse(next_ref, order))


def call(kernel, outs, *args, scratch=(), scalars=0, far=False, limit=24 * 2**20):
    vmem = pl.BlockSpec(memory_space=pltpu.VMEM)
    place_in = pl.BlockSpec(memory_space=pltpu.HBM) if far else vmem
    return pl.pallas_call(
        kernel,
        out_shape=outs,
        in_specs=[pl.BlockSpec(memory_space=pltpu.SMEM)] * scalars + [place_in] * (len(args) - scalars),
        out_specs=[vmem] * len(outs),
        scratch_shapes=list(scratch),
        compiler_params=pltpu.CompilerParams(vmem_limit_bytes=limit),
    )(*args)


def on_device(rhs, inverse_t, u_factors, v_factors, tile_ranks):
    slots, _, r_cols, order = rhs.shape
    rank = u_factors.shape[4]
    n_row = lax.axis_size("row")
    n_x = lax.axis_size("x")
    n_col = 2 * n_x
    assert slots == 2 and n_row == TURNS * n_col and u_factors.shape[2] == slots * TURNS
    everywhere = ("row", "x", "core")
    lanes = order // n_col
    width = r_cols + (n_row - 2) * rank
    half = r_cols + (n_col - 2) * rank
    assert 2 * half == width
    dims = (n_row, n_col, r_cols, rank, width, half)
    shape = jax.ShapeDtypeStruct
    swap = [(0, 1), (1, 0)]

    rhs_here = rhs[:, 0]
    inv_here = inverse_t[:, 0]
    u_here = u_factors[:, 0, :, 0].reshape(slots, slots, TURNS, rank, order)
    v_here = v_factors[:, 0, :, 0].reshape(slots, slots, TURNS, rank, order)
    ranks = jnp.swapaxes(tile_ranks, 2, 3)

    def gather(part):
        pieces = []
        for s in range(n_x):
            moved = part
            if s:
                moved = lax.ppermute(part, "x", [(i, (i + s) % n_x) for i in range(n_x)])
            pieces += [moved, lax.ppermute(moved, "core", swap)]
        return pieces

    def turn_rows(parts):
        got = []
        for s in range(TURNS):
            pairs = []
            for t in range(TURNS):
                for c in range(n_col):
                    for q in range(n_col):
                        pairs.append(((t * n_col + c) * n_col + q, (((t + s) % TURNS) * n_col + q) * n_col + c))
            got.append(lax.ppermute(parts[s], everywhere, pairs))
        return got

    def spread(m):
        same = lax.all_to_all(m, ("row", "x"), split_axis=0, concat_axis=0, tiled=True)
        return same, lax.ppermute(same, "core", swap)

    def kernel(body):
        return functools.partial(body, dims)

    u_rows = n_col * TURNS * rank
    messages = shape((n_row * n_x, rank, width), BF)
    far_shape = shape((rank, width + rank), BF)
    near_scratch = pltpu.VMEM((n_col, order + u_rows, lanes), BF)
    next_scratch = pltpu.VMEM((n_col, order + 2 * u_rows + 4 * r_cols, lanes), BF)
    solve_scratch = [
        pltpu.VMEM((2, n_row * n_x, rank, width), BF),
        pltpu.VMEM((n_row, width + rank, r_cols), BF),
    ]

    v_send = shape((3, rank, order), BF)
    v_a, v_b, near = call(
        kernel(prep_kernel),
        [v_send, v_send, shape((order + u_rows, lanes), BF)],
        ranks, inv_here, u_here, v_here, scalars=1, far=True, limit=67043328 - 450 * 1024,
        scratch=[
            pltpu.VMEM((order, lanes), F32),
            pltpu.VMEM((TURNS, rank, order), BF),
            pltpu.VMEM((slots, slots, TURNS, rank, order), BF),
            pltpu.SemaphoreType.DMA((3,)),
        ],
    )
    near = gather(near)
    v_a, v_b = turn_rows([v_a, v_b])
    msg, far_a, far_b = call(
        kernel(first_kernel), [messages, far_shape, far_shape],
        rhs_here, v_a, v_b, *near, scratch=[near_scratch],
    )

    rhs_late, inv_late, later_u, msg, far_a, far_b = lax.optimization_barrier(
        (rhs_here, inv_here, u_here[1], msg, far_a, far_b))
    far = gather(jnp.stack(turn_rows([far_a, far_b])))
    z = lax.dot_general(rhs_late, inv_late, (((2,), (1,)), ((0,), (0,))), precision=lax.Precision.HIGHEST,
                        preferred_element_type=F32)
    z_high = lax.reduce_precision(z, 8, 7)
    z_low = z - z_high
    later_u = later_u.reshape(slots, TURNS * rank, order)
    nxt = gather(jnp.concatenate([inv_late[1].astype(BF)] + [
        later_u[a, :, m * lanes : (m + 1) * lanes] for a in range(slots) for m in range(n_col)] + [
        part[a].astype(BF) for a in range(slots) for part in (z_high, z_low)], axis=0))
    same, other = spread(msg)

    msg, minus, own = call(
        kernel(middle_kernel),
        [messages, shape((r_cols, order), F32), shape((width + rank - r_cols, r_cols), BF)],
        same, other, rhs_here, v_a, v_b, *far, *nxt,
        scratch=solve_scratch + [pltpu.VMEM((n_col, TURNS, rank, width + rank), BF), next_scratch],
    )
    same, other = spread(msg)
    (early,) = call(
        kernel(early_kernel), [shape((r_cols, order), F32)], own, *near, *nxt,
        scratch=[near_scratch, next_scratch])
    (y,) = call(
        kernel(last_kernel), [shape((slots, r_cols, order), F32)],
        same, other, minus, early, *nxt, scratch=solve_scratch + [next_scratch],
    )
    return y[:, None]


def solution(mesh):
    n_row, n_col = (mesh.shape[name] for name in ("row", "col"))
    fine = Mesh(mesh.devices.reshape(n_row, n_col // 2, 2), ("row", "x", "core"))
    col = ("x", "core")
    in_specs = (
        P(None, "row", None, None),
        P(None, "row", None, col),
        P(None, "row", None, col, None, None),
        P(None, "row", None, col, None, None),
        P(None, "row", None, col),
    )
    out_specs = P(None, "row", None, None)
    return jax.shard_map(on_device, mesh=fine, in_specs=in_specs, out_specs=out_specs, check_vma=False)
```

```python
import functools

import jax
import jax.numpy as jnp
from jax import lax
from jax.experimental import pallas as pl
from jax.experimental.pallas import tpu as pltpu
from jax.sharding import Mesh
from jax.sharding import PartitionSpec as P

BF = jnp.bfloat16
F32 = jnp.float32
NT = (((1,), (1,)), ((), ()))
TN = (((0,), (0,)), ((), ()))
TURNS = 2


def mm(a, b):
    return jnp.dot(a, b, preferred_element_type=F32)


def split_mm(a, b):
    high = a.astype(BF)
    low = (a - high.astype(F32)).astype(BF)
    return mm(high, b) + mm(low, b)


def pack(low, high, both, half):
    return jnp.concatenate([high[:, :half], jnp.where(both, low[:, :half], high[:, half:])], axis=1)


def place():
    row, x, core = lax.axis_index("row"), lax.axis_index("x"), lax.axis_index("core")
    n_col = lax.axis_size("x") * lax.axis_size("core")
    return row, x * lax.axis_size("core") + core, row // n_col


def join(scratch, pieces):
    x, core, n_x = lax.axis_index("x"), lax.axis_index("core"), lax.axis_size("x")
    for s in range(n_x):
        for other in range(2):
            source = lax.rem(x - s + n_x, n_x) * 2 + (1 - core if other else core)
            scratch[source] = pieces[2 * s + other][...]


def put_columns(out_ref, at, rows, block):
    lanes = out_ref.shape[1]
    count = block.shape[1] // lanes
    for m in range(count):
        out_ref[at + m * rows : at + (m + 1) * rows, :] = block[:, m * lanes : (m + 1) * lanes]


def columns(ref, source, at, rows, start, stop, count):
    return jnp.concatenate([ref[source, at + m * rows + start : at + m * rows + stop, :] for m in range(count)], axis=1)


def near_kernel(dims, inv_ref, u_ref, near_ref):
    _, _, _, rank, _, _ = dims
    order = inv_ref.shape[1]
    near_ref[:order, :] = inv_ref[0].astype(BF)
    put_columns(near_ref, order, TURNS * rank, u_ref[0, 0].reshape(TURNS * rank, order))


def mask_kernel(dims, ranks_ref, v_ref, send_a_ref, send_b_ref, later_a_ref, later_b_ref):
    _, _, turn = place()
    rank_rows = lax.broadcasted_iota(jnp.int32, v_ref.shape[3:], 0)

    def masked(i, k, t):
        v = v_ref[i, k, t]
        return jnp.where(rank_rows < ranks_ref[i, 0, 0, k * TURNS + t], v, jnp.zeros_like(v))

    for s, (send_ref, later_ref) in enumerate(((send_a_ref, later_a_ref), (send_b_ref, later_b_ref))):
        t = lax.rem(turn + s, TURNS)
        send_ref[0] = masked(0, 0, t)
        send_ref[1] = masked(1, 0, t)
        later_ref[...] = masked(1, 1, t)


def gathered_inverse(ref, order):
    return jnp.concatenate([ref[c, :order, :] for c in range(ref.shape[0])], axis=1)


def gathered_u(ref, at, rank, blocks):
    n_col = ref.shape[0]
    return jnp.concatenate(
        [columns(ref, j % n_col, at, TURNS * rank, (j // n_col) * rank, (j // n_col + 1) * rank, n_col)
         for j in range(blocks)], axis=0)


def first_kernel(dims, *refs):
    n_row, _, _, rank, width, half = dims
    rhs_ref, v_a_ref, v_b_ref, later_a_ref, later_b_ref = refs[:5]
    msg_ref, far_a_ref, far_b_ref, near_ref = refs[-4:]
    row, col, turn = place()
    order = rhs_ref.shape[2]
    join(near_ref, refs[5:-4])
    inv = gathered_inverse(near_ref, order)
    z = split_mm(rhs_ref[0], inv)
    w = mm(gathered_u(near_ref, order, rank, n_row - 1), inv)
    x = jnp.concatenate([z.astype(BF), w.astype(BF)], axis=0)
    tiles = []
    for v_ref in (v_a_ref, v_b_ref):
        v = v_ref[...].reshape(2 * rank, order)
        tiles.append(lax.dot_general(v, x, NT, preferred_element_type=F32).astype(BF))
    straight = turn == 0
    low = jnp.where(straight, tiles[0][:rank, :width], tiles[1][:rank, :width])
    high = jnp.where(straight, tiles[1][:rank, :width], tiles[0][:rank, :width])
    for n, (far_ref, later_ref) in enumerate(((far_a_ref, later_a_ref), (far_b_ref, later_b_ref))):
        far_ref[:, order : order + width + rank] = tiles[n][rank:]
        far_ref[:, :order] = later_ref[...]
    msg = pack(low, high, col > row, half)
    for d in range(msg_ref.shape[0]):
        msg_ref[d] = msg


def start_solve(q_ref, n_row, r_cols):
    q_ref[...] = jnp.zeros(q_ref.shape, BF)
    eye = (
        lax.broadcasted_iota(jnp.int32, (r_cols, r_cols), 0)
        == lax.broadcasted_iota(jnp.int32, (r_cols, r_cols), 1)
    ).astype(BF)
    for k in range(n_row):
        q_ref[k, :r_cols, :] = eye


def solve(dims, same_ref, other_ref, g_ref, q_ref, extra):
    n_row, n_col, r_cols, rank, width, half = dims
    core = lax.axis_index("core")
    g_ref[core] = same_ref[...]
    g_ref[1 - core] = other_ref[...]
    start_solve(q_ref, n_row, r_cols)
    extras = []
    for k in range(n_row):
        parts = []
        w = half if k <= n_col - 2 else width
        for i in range(k + 1, n_row):
            c, t = i % n_col, i // n_col
            at = half if t == 0 else 0
            parts.append(g_ref[c % 2, k * (n_col // 2) + c // 2, :, at : at + w])
        if extra is not None:
            if k == n_row - 1:
                w = width + rank
            parts.append(extra(k)[:, :w])
        if not parts:
            break
        a = parts[0] if len(parts) == 1 else jnp.concatenate(parts, axis=0)
        new = mm(a, q_ref[k, :w, :])
        for i in range(k + 1, n_row):
            at = (i - k - 1) * rank
            q_ref[i, r_cols + k * rank : r_cols + (k + 1) * rank, :] = (-new[at : at + rank]).astype(BF)
        if extra is not None:
            extras.append(new[(n_row - 1 - k) * rank :].astype(BF))
    return extras


def middle_kernel(dims, *refs):
    n_row, n_col, r_cols, rank, _, half = dims
    same_ref, other_ref, rhs_ref, v_a_ref, v_b_ref = refs[:5]
    fars, nexts = refs[5 : 5 + n_col], refs[5 + n_col : 5 + 2 * n_col]
    msg_ref, minus_ref, own_ref, g_ref, q_ref, far_ref, next_ref = refs[5 + 2 * n_col :]
    row, col, turn = place()
    order = rhs_ref.shape[2]
    rows = n_col * TURNS * rank
    join(next_ref, nexts)
    join(far_ref, fars)
    inv = gathered_inverse(next_ref, order)
    w = mm(gathered_u(next_ref, order + rows, rank, n_row - 2), inv)
    p = solve(dims, same_ref, other_ref, g_ref, q_ref,
              lambda k: far_ref[k % n_col, lax.rem(turn - k // n_col + TURNS, TURNS)])
    total = lax.dot_general(jnp.concatenate(p, axis=0), gathered_u(next_ref, order, rank, n_row), TN,
                            preferred_element_type=F32)
    z = split_mm(rhs_ref[1] - total, inv)
    minus_ref[...] = -total
    x = jnp.concatenate([z.astype(BF), w.astype(BF)], axis=0)
    tiles = [lax.dot_general(v_ref[:, :order], x, NT, preferred_element_type=F32).astype(BF) for v_ref in (v_a_ref, v_b_ref)]
    straight = turn == 0
    low = jnp.where(straight, tiles[0], tiles[1])
    high = jnp.where(straight, tiles[1], tiles[0])
    msg = pack(low, high, col > row, half)
    for d in range(msg_ref.shape[0]):
        msg_ref[d] = msg
    own_ref[...] = q_ref[row][r_cols:, :]


def early_kernel(dims, *refs):
    n_row, n_col, _, rank, _, _ = dims
    own_ref = refs[0]
    nears, zs = refs[1 : 1 + n_col], refs[1 + n_col : 1 + 2 * n_col]
    y_ref, z_out_ref, near_ref, z_ref = refs[1 + 2 * n_col :]
    order = y_ref.shape[1]
    join(near_ref, nears)
    join(z_ref, zs)
    minus = lax.dot_general(own_ref[...], gathered_u(near_ref, order, rank, n_row - 1), TN, preferred_element_type=F32)
    z = jnp.concatenate([z_ref[c, 0] for c in range(n_col)], axis=1)
    y_ref[...] = z + split_mm(minus, gathered_inverse(near_ref, order))
    z_out_ref[...] = jnp.concatenate([z_ref[c, 1] for c in range(n_col)], axis=1)


def last_kernel(dims, *refs):
    n_row, n_col, r_cols, rank, _, _ = dims
    same_ref, other_ref, minus_ref, z_ref, early_ref = refs[:5]
    y_ref, g_ref, q_ref, next_ref = refs[5 + n_col :]
    order = minus_ref.shape[1]
    y_ref[0] = early_ref[...]
    join(next_ref, refs[5 : 5 + n_col])
    solve(dims, same_ref, other_ref, g_ref, q_ref, None)
    own = q_ref[lax.axis_index("row")][r_cols:, :]
    u = gathered_u(next_ref, order + n_col * TURNS * rank, rank, n_row - 1)
    minus = minus_ref[...] + lax.dot_general(own, u, TN, preferred_element_type=F32)
    y_ref[1] = z_ref[...] + split_mm(minus, gathered_inverse(next_ref, order))


def call(kernel, outs, *args, scratch=(), scalars=0):
    vmem = pl.BlockSpec(memory_space=pltpu.VMEM)
    return pl.pallas_call(
        kernel,
        out_shape=outs,
        in_specs=[pl.BlockSpec(memory_space=pltpu.SMEM)] * scalars + [vmem] * (len(args) - scalars),
        out_specs=[vmem] * len(outs),
        scratch_shapes=list(scratch),
        compiler_params=pltpu.CompilerParams(vmem_limit_bytes=24 * 2**20),
    )(*args)


def on_device(rhs, inverse_t, u_factors, v_factors, tile_ranks):
    slots, _, r_cols, order = rhs.shape
    rank = u_factors.shape[4]
    n_row = lax.axis_size("row")
    n_x = lax.axis_size("x")
    n_col = 2 * n_x
    assert slots == 2 and n_row == TURNS * n_col and u_factors.shape[2] == slots * TURNS
    everywhere = ("row", "x", "core")
    lanes = order // n_col
    width = r_cols + (n_row - 2) * rank
    half = r_cols + (n_col - 2) * rank
    assert 2 * half == width
    dims = (n_row, n_col, r_cols, rank, width, half)
    shape = jax.ShapeDtypeStruct
    swap = [(0, 1), (1, 0)]

    rhs_here = rhs[:, 0]
    inv_here = inverse_t[:, 0]
    u_here = u_factors[:, 0, :, 0].reshape(slots, slots, TURNS, rank, order)
    v_here = v_factors[:, 0, :, 0].reshape(slots, slots, TURNS, rank, order)
    ranks = jnp.swapaxes(tile_ranks, 2, 3)

    def gather(part):
        pieces = []
        for s in range(n_x):
            moved = part
            if s:
                moved = lax.ppermute(part, "x", [(i, (i + s) % n_x) for i in range(n_x)])
            pieces += [moved, lax.ppermute(moved, "core", swap)]
        return pieces

    def turn_rows(parts):
        got = []
        for s in range(TURNS):
            pairs = []
            for t in range(TURNS):
                for c in range(n_col):
                    for q in range(n_col):
                        pairs.append(((t * n_col + c) * n_col + q, (((t + s) % TURNS) * n_col + q) * n_col + c))
            got.append(lax.ppermute(parts[s], everywhere, pairs))
        return got

    def spread(m):
        same = lax.all_to_all(m, ("row", "x"), split_axis=0, concat_axis=0, tiled=True)
        return same, lax.ppermute(same, "core", swap)

    def kernel(body):
        return functools.partial(body, dims)

    u_rows = n_col * TURNS * rank
    messages = shape((n_row * n_x, rank, width), BF)
    far_shape = shape((rank, order + width + rank), BF)
    near_scratch = pltpu.VMEM((n_col, order + u_rows, lanes), BF)
    next_scratch = pltpu.VMEM((n_col, order + 2 * u_rows, lanes), BF)
    solve_scratch = [
        pltpu.VMEM((2, n_row * n_x, rank, width), BF),
        pltpu.VMEM((n_row, width + rank, r_cols), BF),
    ]

    (near,) = call(kernel(near_kernel), [shape((order + u_rows, lanes), BF)], inv_here, u_here)
    v_a, v_b, later_a, later_b = call(
        kernel(mask_kernel),
        [shape((2, rank, order), BF)] * 2 + [shape((rank, order), BF)] * 2,
        ranks, v_here, scalars=1,
    )
    near = gather(near)
    v_a, v_b = turn_rows([v_a, v_b])
    later_u = u_here[1].reshape(slots, TURNS * rank, order)
    nxt = gather(jnp.concatenate([inv_here[1].astype(BF)] + [
        later_u[a, :, m * lanes : (m + 1) * lanes] for a in range(slots) for m in range(n_col)], axis=0))

    msg, far_a, far_b = call(
        kernel(first_kernel), [messages, far_shape, far_shape],
        rhs_here, v_a, v_b, later_a, later_b, *near, scratch=[near_scratch],
    )

    rhs_late, inv_late, msg, far_a, far_b = lax.optimization_barrier((rhs_here, inv_here, msg, far_a, far_b))
    later_a, later_b = turn_rows([far_a, far_b])
    far = gather(jnp.stack([later_a, later_b])[:, :, order:])
    same, other = spread(msg)
    z = gather(lax.dot_general(rhs_late, inv_late, (((2,), (1,)), ((0,), (0,))), precision=lax.Precision.HIGHEST,
                               preferred_element_type=F32))

    msg, minus, own = call(
        kernel(middle_kernel),
        [messages, shape((r_cols, order), F32), shape((width + rank - r_cols, r_cols), BF)],
        same, other, rhs_here, later_a, later_b, *far, *nxt,
        scratch=solve_scratch + [pltpu.VMEM((n_col, TURNS, rank, width + rank), BF), next_scratch],
    )
    same, other = spread(msg)
    early, z_last = call(
        kernel(early_kernel), [shape((r_cols, order), F32)] * 2, own, *near, *z,
        scratch=[near_scratch, pltpu.VMEM((n_col, slots, r_cols, lanes), F32)])
    (y,) = call(
        kernel(last_kernel), [shape((slots, r_cols, order), F32)],
        same, other, minus, z_last, early, *nxt, scratch=solve_scratch + [next_scratch],
    )
    return y[:, None]


def solution(mesh):
    n_row, n_col = (mesh.shape[name] for name in ("row", "col"))
    fine = Mesh(mesh.devices.reshape(n_row, n_col // 2, 2), ("row", "x", "core"))
    col = ("x", "core")
    in_specs = (
        P(None, "row", None, None),
        P(None, "row", None, col),
        P(None, "row", None, col, None, None),
        P(None, "row", None, col, None, None),
        P(None, "row", None, col),
    )
    out_specs = P(None, "row", None, None)
    return jax.shard_map(on_device, mesh=fine, in_specs=in_specs, out_specs=out_specs, check_vma=False)
```

```python
import functools

import jax
import jax.numpy as jnp
from jax import lax
from jax.experimental import pallas as pl
from jax.experimental.pallas import tpu as pltpu
from jax.sharding import Mesh
from jax.sharding import PartitionSpec as P

BF = jnp.bfloat16
F32 = jnp.float32
NT = (((1,), (1,)), ((), ()))
TN = (((0,), (0,)), ((), ()))
TURNS = 2


def mm(a, b):
    return jnp.dot(a, b, preferred_element_type=F32)


def split_mm(a, b):
    high = a.astype(BF)
    low = (a - high.astype(F32)).astype(BF)
    return mm(high, b) + mm(low, b)


def pack(low, high, both, half):
    return jnp.concatenate([high[:, :half], jnp.where(both, low[:, :half], high[:, half:])], axis=1)


def place():
    row, x, core = lax.axis_index("row"), lax.axis_index("x"), lax.axis_index("core")
    n_col = lax.axis_size("x") * lax.axis_size("core")
    return row, x * lax.axis_size("core") + core, row // n_col


def join(scratch, pieces):
    x, core, n_x = lax.axis_index("x"), lax.axis_index("core"), lax.axis_size("x")
    for s in range(n_x):
        for other in range(2):
            source = lax.rem(x - s + n_x, n_x) * 2 + (1 - core if other else core)
            scratch[source] = pieces[2 * s + other][...]


def put_columns(out_ref, at, rows, block):
    lanes = out_ref.shape[1]
    count = block.shape[1] // lanes
    for m in range(count):
        out_ref[at + m * rows : at + (m + 1) * rows, :] = block[:, m * lanes : (m + 1) * lanes]


def columns(ref, source, at, rows, start, stop, count):
    return jnp.concatenate([ref[source, at + m * rows + start : at + m * rows + stop, :] for m in range(count)], axis=1)


def near_kernel(dims, inv_ref, u_ref, near_ref):
    _, _, _, rank, _, _ = dims
    order = inv_ref.shape[1]
    near_ref[:order, :] = inv_ref[0].astype(BF)
    put_columns(near_ref, order, TURNS * rank, u_ref[0, 0].reshape(TURNS * rank, order))


def mask_kernel(dims, ranks_ref, v_ref, send_a_ref, send_b_ref, later_a_ref, later_b_ref):
    _, _, turn = place()
    rank_rows = lax.broadcasted_iota(jnp.int32, v_ref.shape[3:], 0)

    def masked(i, k, t):
        v = v_ref[i, k, t]
        ranks = [ranks_ref[i, 0, :, k * TURNS + n : k * TURNS + n + 1] for n in range(TURNS)]
        return jnp.where(rank_rows < jnp.where(t == 0, *ranks), v, jnp.zeros_like(v))

    for s, (send_ref, later_ref) in enumerate(((send_a_ref, later_a_ref), (send_b_ref, later_b_ref))):
        t = lax.rem(turn + s, TURNS)
        send_ref[0] = masked(0, 0, t)
        send_ref[1] = masked(1, 0, t)
        later_ref[...] = masked(1, 1, t)


def gathered_inverse(ref, order):
    return jnp.concatenate([ref[c, :order, :] for c in range(ref.shape[0])], axis=1)


def gathered_u(ref, at, rank, blocks):
    n_col = ref.shape[0]
    return jnp.concatenate(
        [columns(ref, j % n_col, at, TURNS * rank, (j // n_col) * rank, (j // n_col + 1) * rank, n_col)
         for j in range(blocks)], axis=0)


def first_kernel(dims, *refs):
    n_row, _, _, rank, width, half = dims
    rhs_ref, v_a_ref, v_b_ref, later_a_ref, later_b_ref = refs[:5]
    msg_ref, far_a_ref, far_b_ref, near_ref = refs[-4:]
    row, col, turn = place()
    order = rhs_ref.shape[2]
    join(near_ref, refs[5:-4])
    inv = gathered_inverse(near_ref, order)
    z = split_mm(rhs_ref[0], inv)
    w = mm(gathered_u(near_ref, order, rank, n_row - 1), inv)
    x = jnp.concatenate([z.astype(BF), w.astype(BF)], axis=0)
    tiles = []
    for v_ref in (v_a_ref, v_b_ref):
        v = v_ref[...].reshape(2 * rank, order)
        tiles.append(lax.dot_general(v, x, NT, preferred_element_type=F32).astype(BF))
    straight = turn == 0
    low = jnp.where(straight, tiles[0][:rank, :width], tiles[1][:rank, :width])
    high = jnp.where(straight, tiles[1][:rank, :width], tiles[0][:rank, :width])
    for n, (far_ref, later_ref) in enumerate(((far_a_ref, later_a_ref), (far_b_ref, later_b_ref))):
        far_ref[:, order : order + width + rank] = tiles[n][rank:]
        far_ref[:, :order] = later_ref[...]
    msg = pack(low, high, col > row, half)
    for d in range(msg_ref.shape[0]):
        msg_ref[d] = msg


def start_solve(q_ref, n_row, r_cols):
    q_ref[...] = jnp.zeros(q_ref.shape, BF)
    eye = (
        lax.broadcasted_iota(jnp.int32, (r_cols, r_cols), 0)
        == lax.broadcasted_iota(jnp.int32, (r_cols, r_cols), 1)
    ).astype(BF)
    for k in range(n_row):
        q_ref[k, :r_cols, :] = eye


def solve(dims, same_ref, other_ref, g_ref, q_ref, extra):
    n_row, n_col, r_cols, rank, width, half = dims
    core = lax.axis_index("core")
    g_ref[core] = same_ref[...]
    g_ref[1 - core] = other_ref[...]
    start_solve(q_ref, n_row, r_cols)
    extras = []
    for k in range(n_row):
        parts = []
        w = half if k <= n_col - 2 else width
        for i in range(k + 1, n_row):
            c, t = i % n_col, i // n_col
            at = half if t == 0 else 0
            parts.append(g_ref[c % 2, k * (n_col // 2) + c // 2, :, at : at + w])
        if extra is not None:
            if k == n_row - 1:
                w = width + rank
            parts.append(extra(k)[:, :w])
        if not parts:
            break
        a = parts[0] if len(parts) == 1 else jnp.concatenate(parts, axis=0)
        new = mm(a, q_ref[k, :w, :])
        for i in range(k + 1, n_row):
            at = (i - k - 1) * rank
            q_ref[i, r_cols + k * rank : r_cols + (k + 1) * rank, :] = (-new[at : at + rank]).astype(BF)
        if extra is not None:
            extras.append(new[(n_row - 1 - k) * rank :].astype(BF))
    return extras


def middle_kernel(dims, *refs):
    n_row, n_col, r_cols, rank, _, half = dims
    same_ref, other_ref, rhs_ref, v_a_ref, v_b_ref = refs[:5]
    fars, nexts = refs[5 : 5 + n_col], refs[5 + n_col : 5 + 2 * n_col]
    msg_ref, minus_ref, own_ref, g_ref, q_ref, far_ref, next_ref = refs[5 + 2 * n_col :]
    row, col, turn = place()
    order = rhs_ref.shape[2]
    rows = n_col * TURNS * rank
    join(next_ref, nexts)
    join(far_ref, fars)
    inv = gathered_inverse(next_ref, order)
    w = mm(gathered_u(next_ref, order + rows, rank, n_row - 2), inv)
    p = solve(dims, same_ref, other_ref, g_ref, q_ref,
              lambda k: far_ref[k % n_col, lax.rem(turn - k // n_col + TURNS, TURNS)])
    total = lax.dot_general(jnp.concatenate(p, axis=0), gathered_u(next_ref, order, rank, n_row), TN,
                            preferred_element_type=F32)
    z = split_mm(rhs_ref[1] - total, inv)
    minus_ref[...] = -total
    x = jnp.concatenate([z.astype(BF), w.astype(BF)], axis=0)
    tiles = [lax.dot_general(v_ref[:, :order], x, NT, preferred_element_type=F32).astype(BF) for v_ref in (v_a_ref, v_b_ref)]
    straight = turn == 0
    low = jnp.where(straight, tiles[0], tiles[1])
    high = jnp.where(straight, tiles[1], tiles[0])
    msg = pack(low, high, col > row, half)
    for d in range(msg_ref.shape[0]):
        msg_ref[d] = msg
    own_ref[...] = q_ref[row][r_cols:, :]


def early_kernel(dims, *refs):
    n_row, n_col, _, rank, _, _ = dims
    own_ref = refs[0]
    nears, zs = refs[1 : 1 + n_col], refs[1 + n_col : 1 + 2 * n_col]
    y_ref, z_out_ref, near_ref, z_ref = refs[1 + 2 * n_col :]
    order = y_ref.shape[1]
    join(near_ref, nears)
    join(z_ref, zs)
    minus = lax.dot_general(own_ref[...], gathered_u(near_ref, order, rank, n_row - 1), TN, preferred_element_type=F32)
    z = jnp.concatenate([z_ref[c, 0] for c in range(n_col)], axis=1)
    y_ref[...] = z + split_mm(minus, gathered_inverse(near_ref, order))
    z_out_ref[...] = jnp.concatenate([z_ref[c, 1] for c in range(n_col)], axis=1)


def last_kernel(dims, *refs):
    n_row, n_col, r_cols, rank, _, _ = dims
    same_ref, other_ref, minus_ref, z_ref, early_ref = refs[:5]
    y_ref, g_ref, q_ref, next_ref = refs[5 + n_col :]
    order = minus_ref.shape[1]
    y_ref[0] = early_ref[...]
    join(next_ref, refs[5 : 5 + n_col])
    solve(dims, same_ref, other_ref, g_ref, q_ref, None)
    own = q_ref[lax.axis_index("row")][r_cols:, :]
    u = gathered_u(next_ref, order + n_col * TURNS * rank, rank, n_row - 1)
    minus = minus_ref[...] + lax.dot_general(own, u, TN, preferred_element_type=F32)
    y_ref[1] = z_ref[...] + split_mm(minus, gathered_inverse(next_ref, order))


def call(kernel, outs, *args, scratch=()):
    vmem = pl.BlockSpec(memory_space=pltpu.VMEM)
    return pl.pallas_call(
        kernel,
        out_shape=outs,
        in_specs=[vmem] * len(args),
        out_specs=[vmem] * len(outs),
        scratch_shapes=list(scratch),
        compiler_params=pltpu.CompilerParams(vmem_limit_bytes=24 * 2**20),
    )(*args)


def on_device(rhs, inverse_t, u_factors, v_factors, tile_ranks):
    slots, _, r_cols, order = rhs.shape
    rank = u_factors.shape[4]
    n_row = lax.axis_size("row")
    n_x = lax.axis_size("x")
    n_col = 2 * n_x
    assert slots == 2 and n_row == TURNS * n_col and u_factors.shape[2] == slots * TURNS
    everywhere = ("row", "x", "core")
    lanes = order // n_col
    width = r_cols + (n_row - 2) * rank
    half = r_cols + (n_col - 2) * rank
    assert 2 * half == width
    dims = (n_row, n_col, r_cols, rank, width, half)
    shape = jax.ShapeDtypeStruct
    swap = [(0, 1), (1, 0)]

    rhs_here = rhs[:, 0]
    inv_here = inverse_t[:, 0]
    u_here = u_factors[:, 0, :, 0].reshape(slots, slots, TURNS, rank, order)
    v_here = v_factors[:, 0, :, 0].reshape(slots, slots, TURNS, rank, order)
    ranks = jnp.swapaxes(tile_ranks, 2, 3)

    def gather(part):
        pieces = []
        for s in range(n_x):
            moved = part
            if s:
                moved = lax.ppermute(part, "x", [(i, (i + s) % n_x) for i in range(n_x)])
            pieces += [moved, lax.ppermute(moved, "core", swap)]
        return pieces

    def turn_rows(parts):
        got = []
        for s in range(TURNS):
            pairs = []
            for t in range(TURNS):
                for c in range(n_col):
                    for q in range(n_col):
                        pairs.append(((t * n_col + c) * n_col + q, (((t + s) % TURNS) * n_col + q) * n_col + c))
            got.append(lax.ppermute(parts[s], everywhere, pairs))
        return got

    def spread(m):
        same = lax.all_to_all(m, ("row", "x"), split_axis=0, concat_axis=0, tiled=True)
        return same, lax.ppermute(same, "core", swap)

    def kernel(body):
        return functools.partial(body, dims)

    u_rows = n_col * TURNS * rank
    messages = shape((n_row * n_x, rank, width), BF)
    far_shape = shape((rank, order + width + rank), BF)
    near_scratch = pltpu.VMEM((n_col, order + u_rows, lanes), BF)
    next_scratch = pltpu.VMEM((n_col, order + 2 * u_rows, lanes), BF)
    solve_scratch = [
        pltpu.VMEM((2, n_row * n_x, rank, width), BF),
        pltpu.VMEM((n_row, width + rank, r_cols), BF),
    ]

    (near,) = call(kernel(near_kernel), [shape((order + u_rows, lanes), BF)], inv_here, u_here)
    v_a, v_b, later_a, later_b = call(
        kernel(mask_kernel),
        [shape((2, rank, order), BF)] * 2 + [shape((rank, order), BF)] * 2,
        ranks, v_here,
    )
    near = gather(near)
    v_a, v_b = turn_rows([v_a, v_b])
    later_u = u_here[1].reshape(slots, TURNS * rank, order)
    nxt = gather(jnp.concatenate([inv_here[1].astype(BF)] + [
        later_u[a, :, m * lanes : (m + 1) * lanes] for a in range(slots) for m in range(n_col)], axis=0))

    msg, far_a, far_b = call(
        kernel(first_kernel), [messages, far_shape, far_shape],
        rhs_here, v_a, v_b, later_a, later_b, *near, scratch=[near_scratch],
    )

    rhs_late, inv_late, msg, far_a, far_b = lax.optimization_barrier((rhs_here, inv_here, msg, far_a, far_b))
    later_a, later_b = turn_rows([far_a, far_b])
    far = gather(jnp.stack([later_a, later_b])[:, :, order:])
    same, other = spread(msg)
    z = gather(lax.dot_general(rhs_late, inv_late, (((2,), (1,)), ((0,), (0,))), precision=lax.Precision.HIGHEST,
                               preferred_element_type=F32))

    msg, minus, own = call(
        kernel(middle_kernel),
        [messages, shape((r_cols, order), F32), shape((width + rank - r_cols, r_cols), BF)],
        same, other, rhs_here, later_a, later_b, *far, *nxt,
        scratch=solve_scratch + [pltpu.VMEM((n_col, TURNS, rank, width + rank), BF), next_scratch],
    )
    same, other = spread(msg)
    early, z_last = call(
        kernel(early_kernel), [shape((r_cols, order), F32)] * 2, own, *near, *z,
        scratch=[near_scratch, pltpu.VMEM((n_col, slots, r_cols, lanes), F32)])
    (y,) = call(
        kernel(last_kernel), [shape((slots, r_cols, order), F32)],
        same, other, minus, z_last, early, *nxt, scratch=solve_scratch + [next_scratch],
    )
    return y[:, None]


def solution(mesh):
    n_row, n_col = (mesh.shape[name] for name in ("row", "col"))
    fine = Mesh(mesh.devices.reshape(n_row, n_col // 2, 2), ("row", "x", "core"))
    col = ("x", "core")
    in_specs = (
        P(None, "row", None, None),
        P(None, "row", None, col),
        P(None, "row", None, col, None, None),
        P(None, "row", None, col, None, None),
        P(None, "row", None, col),
    )
    out_specs = P(None, "row", None, None)
    return jax.shard_map(on_device, mesh=fine, in_specs=in_specs, out_specs=out_specs, check_vma=False)
```

```python
import functools

import jax
import jax.numpy as jnp
from jax import lax
from jax.experimental import pallas as pl
from jax.experimental.pallas import tpu as pltpu
from jax.sharding import Mesh
from jax.sharding import PartitionSpec as P

BF = jnp.bfloat16
F32 = jnp.float32
NT = (((1,), (1,)), ((), ()))
TN = (((0,), (0,)), ((), ()))
TURNS = 2


def mm(a, b):
    return jnp.dot(a, b, preferred_element_type=F32)


def split_mm(a, b):
    high = a.astype(BF)
    low = (a - high.astype(F32)).astype(BF)
    return mm(high, b) + mm(low, b)


def pack(low, high, both, half):
    return jnp.concatenate([high[:, :half], jnp.where(both, low[:, :half], high[:, half:])], axis=1)


def place():
    row, x, core = lax.axis_index("row"), lax.axis_index("x"), lax.axis_index("core")
    n_col = lax.axis_size("x") * lax.axis_size("core")
    return row, x * lax.axis_size("core") + core, row // n_col


def join(scratch, pieces):
    x, core, n_x = lax.axis_index("x"), lax.axis_index("core"), lax.axis_size("x")
    for s in range(n_x):
        for other in range(2):
            source = lax.rem(x - s + n_x, n_x) * 2 + (1 - core if other else core)
            scratch[source] = pieces[2 * s + other][...]


def put_columns(out_ref, at, rows, block):
    lanes = out_ref.shape[1]
    count = block.shape[1] // lanes
    for m in range(count):
        out_ref[at + m * rows : at + (m + 1) * rows, :] = block[:, m * lanes : (m + 1) * lanes]


def columns(ref, source, at, rows, start, stop, count):
    return jnp.concatenate([ref[source, at + m * rows + start : at + m * rows + stop, :] for m in range(count)], axis=1)


def prep_kernel(dims, ranks_hbm, inv_hbm, u_hbm, v_hbm, near_ref, send_a_ref, send_b_ref, later_a_ref, later_b_ref,
                ranks_ref, inv_ref, u_ref, v_ref, sems):
    _, _, _, rank, _, _ = dims
    _, _, turn = place()
    order = inv_ref.shape[0]
    copies = [
        pltpu.make_async_copy(inv_hbm.at[0], inv_ref, sems.at[0]),
        pltpu.make_async_copy(u_hbm.at[0, 0], u_ref, sems.at[1]),
        pltpu.make_async_copy(v_hbm, v_ref, sems.at[2]),
        pltpu.make_async_copy(ranks_hbm, ranks_ref, sems.at[3]),
    ]
    for copy in copies:
        copy.start()
    copies[0].wait()
    copies[1].wait()
    near_ref[:order, :] = inv_ref[...].astype(BF)
    put_columns(near_ref, order, TURNS * rank, u_ref[...].reshape(TURNS * rank, order))
    copies[2].wait()
    copies[3].wait()
    rank_rows = lax.broadcasted_iota(jnp.int32, v_ref.shape[3:], 0)

    def masked(i, k, t):
        v = v_ref[i, k, t]
        return jnp.where(rank_rows < ranks_ref[i, 0, 0, k * TURNS + t], v, jnp.zeros_like(v))

    for s, (send_ref, later_ref) in enumerate(((send_a_ref, later_a_ref), (send_b_ref, later_b_ref))):
        t = lax.rem(turn + s, TURNS)
        send_ref[0] = masked(0, 0, t)
        send_ref[1] = masked(1, 0, t)
        later_ref[...] = masked(1, 1, t)


def gathered_inverse(ref, order):
    return jnp.concatenate([ref[c, :order, :] for c in range(ref.shape[0])], axis=1)


def gathered_u(ref, at, rank, blocks):
    n_col = ref.shape[0]
    return jnp.concatenate(
        [columns(ref, j % n_col, at, TURNS * rank, (j // n_col) * rank, (j // n_col + 1) * rank, n_col)
         for j in range(blocks)], axis=0)


def first_kernel(dims, *refs):
    n_row, _, _, rank, width, half = dims
    rhs_ref, v_a_ref, v_b_ref, later_a_ref, later_b_ref = refs[:5]
    msg_ref, far_a_ref, far_b_ref, near_ref = refs[-4:]
    row, col, turn = place()
    order = rhs_ref.shape[2]
    join(near_ref, refs[5:-4])
    inv = gathered_inverse(near_ref, order)
    z = split_mm(rhs_ref[0], inv)
    w = mm(gathered_u(near_ref, order, rank, n_row - 1), inv)
    x = jnp.concatenate([z.astype(BF), w.astype(BF)], axis=0)
    tiles = []
    for v_ref in (v_a_ref, v_b_ref):
        v = v_ref[...].reshape(2 * rank, order)
        tiles.append(lax.dot_general(v, x, NT, preferred_element_type=F32).astype(BF))
    straight = turn == 0
    low = jnp.where(straight, tiles[0][:rank, :width], tiles[1][:rank, :width])
    high = jnp.where(straight, tiles[1][:rank, :width], tiles[0][:rank, :width])
    for n, (far_ref, later_ref) in enumerate(((far_a_ref, later_a_ref), (far_b_ref, later_b_ref))):
        far_ref[:, order : order + width + rank] = tiles[n][rank:]
        far_ref[:, :order] = later_ref[...]
    msg = pack(low, high, col > row, half)
    for d in range(msg_ref.shape[0]):
        msg_ref[d] = msg


def start_solve(q_ref, n_row, r_cols):
    q_ref[...] = jnp.zeros(q_ref.shape, BF)
    eye = (
        lax.broadcasted_iota(jnp.int32, (r_cols, r_cols), 0)
        == lax.broadcasted_iota(jnp.int32, (r_cols, r_cols), 1)
    ).astype(BF)
    for k in range(n_row):
        q_ref[k, :r_cols, :] = eye


def solve(dims, same_ref, other_ref, g_ref, q_ref, extra):
    n_row, n_col, r_cols, rank, width, half = dims
    core = lax.axis_index("core")
    g_ref[core] = same_ref[...]
    g_ref[1 - core] = other_ref[...]
    start_solve(q_ref, n_row, r_cols)
    extras = []
    for k in range(n_row):
        parts = []
        w = half if k <= n_col - 2 else width
        for i in range(k + 1, n_row):
            c, t = i % n_col, i // n_col
            at = half if t == 0 else 0
            parts.append(g_ref[c % 2, k * (n_col // 2) + c // 2, :, at : at + w])
        if extra is not None:
            if k == n_row - 1:
                w = width + rank
            parts.append(extra(k)[:, :w])
        if not parts:
            break
        a = parts[0] if len(parts) == 1 else jnp.concatenate(parts, axis=0)
        new = mm(a, q_ref[k, :w, :])
        for i in range(k + 1, n_row):
            at = (i - k - 1) * rank
            q_ref[i, r_cols + k * rank : r_cols + (k + 1) * rank, :] = (-new[at : at + rank]).astype(BF)
        if extra is not None:
            extras.append(new[(n_row - 1 - k) * rank :].astype(BF))
    return extras


def middle_kernel(dims, *refs):
    n_row, n_col, r_cols, rank, _, half = dims
    same_ref, other_ref, rhs_ref, v_a_ref, v_b_ref = refs[:5]
    fars, nexts = refs[5 : 5 + n_col], refs[5 + n_col : 5 + 2 * n_col]
    msg_ref, minus_ref, own_ref, g_ref, q_ref, far_ref, next_ref = refs[5 + 2 * n_col :]
    row, col, turn = place()
    order = rhs_ref.shape[2]
    rows = n_col * TURNS * rank
    join(next_ref, nexts)
    join(far_ref, fars)
    inv = gathered_inverse(next_ref, order)
    w = mm(gathered_u(next_ref, order + rows, rank, n_row - 2), inv)
    p = solve(dims, same_ref, other_ref, g_ref, q_ref,
              lambda k: far_ref[k % n_col, lax.rem(turn - k // n_col + TURNS, TURNS)])
    total = lax.dot_general(jnp.concatenate(p, axis=0), gathered_u(next_ref, order, rank, n_row), TN,
                            preferred_element_type=F32)
    z = split_mm(rhs_ref[1] - total, inv)
    minus_ref[...] = -total
    x = jnp.concatenate([z.astype(BF), w.astype(BF)], axis=0)
    tiles = [lax.dot_general(v_ref[:, :order], x, NT, preferred_element_type=F32).astype(BF) for v_ref in (v_a_ref, v_b_ref)]
    straight = turn == 0
    low = jnp.where(straight, tiles[0], tiles[1])
    high = jnp.where(straight, tiles[1], tiles[0])
    msg = pack(low, high, col > row, half)
    for d in range(msg_ref.shape[0]):
        msg_ref[d] = msg
    own_ref[...] = q_ref[row][r_cols:, :]


def early_kernel(dims, *refs):
    n_row, n_col, _, rank, _, _ = dims
    own_ref = refs[0]
    nears, zs = refs[1 : 1 + n_col], refs[1 + n_col : 1 + 2 * n_col]
    y_ref, z_out_ref, near_ref, z_ref = refs[1 + 2 * n_col :]
    order = y_ref.shape[1]
    join(near_ref, nears)
    join(z_ref, zs)
    minus = lax.dot_general(own_ref[...], gathered_u(near_ref, order, rank, n_row - 1), TN, preferred_element_type=F32)
    z = jnp.concatenate([z_ref[c, 0] for c in range(n_col)], axis=1)
    y_ref[...] = z + split_mm(minus, gathered_inverse(near_ref, order))
    z_out_ref[...] = jnp.concatenate([z_ref[c, 1] for c in range(n_col)], axis=1)


def last_kernel(dims, *refs):
    n_row, n_col, r_cols, rank, _, _ = dims
    same_ref, other_ref, minus_ref, z_ref, early_ref = refs[:5]
    y_ref, g_ref, q_ref, next_ref = refs[5 + n_col :]
    order = minus_ref.shape[1]
    y_ref[0] = early_ref[...]
    join(next_ref, refs[5 : 5 + n_col])
    solve(dims, same_ref, other_ref, g_ref, q_ref, None)
    own = q_ref[lax.axis_index("row")][r_cols:, :]
    u = gathered_u(next_ref, order + n_col * TURNS * rank, rank, n_row - 1)
    minus = minus_ref[...] + lax.dot_general(own, u, TN, preferred_element_type=F32)
    y_ref[1] = z_ref[...] + split_mm(minus, gathered_inverse(next_ref, order))


def call(kernel, outs, *args, scratch=(), space=pltpu.VMEM):
    return pl.pallas_call(
        kernel,
        out_shape=outs,
        in_specs=[pl.BlockSpec(memory_space=space)] * len(args),
        out_specs=[pl.BlockSpec(memory_space=pltpu.VMEM)] * len(outs),
        scratch_shapes=list(scratch),
        compiler_params=pltpu.CompilerParams(vmem_limit_bytes=24 * 2**20),
    )(*args)


def on_device(rhs, inverse_t, u_factors, v_factors, tile_ranks):
    slots, _, r_cols, order = rhs.shape
    rank = u_factors.shape[4]
    n_row = lax.axis_size("row")
    n_x = lax.axis_size("x")
    n_col = 2 * n_x
    assert slots == 2 and n_row == TURNS * n_col and u_factors.shape[2] == slots * TURNS
    everywhere = ("row", "x", "core")
    lanes = order // n_col
    width = r_cols + (n_row - 2) * rank
    half = r_cols + (n_col - 2) * rank
    assert 2 * half == width
    dims = (n_row, n_col, r_cols, rank, width, half)
    shape = jax.ShapeDtypeStruct
    swap = [(0, 1), (1, 0)]

    rhs_here = rhs[:, 0]
    inv_here = inverse_t[:, 0]
    u_here = u_factors[:, 0, :, 0].reshape(slots, slots, TURNS, rank, order)
    v_here = v_factors[:, 0, :, 0].reshape(slots, slots, TURNS, rank, order)
    ranks = jnp.swapaxes(tile_ranks, 2, 3)

    def gather(part):
        pieces = []
        for s in range(n_x):
            moved = part
            if s:
                moved = lax.ppermute(part, "x", [(i, (i + s) % n_x) for i in range(n_x)])
            pieces += [moved, lax.ppermute(moved, "core", swap)]
        return pieces

    def turn_rows(parts):
        got = []
        for s in range(TURNS):
            pairs = []
            for t in range(TURNS):
                for c in range(n_col):
                    for q in range(n_col):
                        pairs.append(((t * n_col + c) * n_col + q, (((t + s) % TURNS) * n_col + q) * n_col + c))
            got.append(lax.ppermute(parts[s], everywhere, pairs))
        return got

    def spread(m):
        same = lax.all_to_all(m, ("row", "x"), split_axis=0, concat_axis=0, tiled=True)
        return same, lax.ppermute(same, "core", swap)

    def kernel(body):
        return functools.partial(body, dims)

    u_rows = n_col * TURNS * rank
    messages = shape((n_row * n_x, rank, width), BF)
    far_shape = shape((rank, order + width + rank), BF)
    near_scratch = pltpu.VMEM((n_col, order + u_rows, lanes), BF)
    next_scratch = pltpu.VMEM((n_col, order + 2 * u_rows, lanes), BF)
    solve_scratch = [
        pltpu.VMEM((2, n_row * n_x, rank, width), BF),
        pltpu.VMEM((n_row, width + rank, r_cols), BF),
    ]

    in_hbm = [pltpu.with_memory_space_constraint(x, pltpu.HBM) for x in (ranks, inv_here, u_here, v_here)]
    near, v_a, v_b, later_a, later_b = call(
        kernel(prep_kernel),
        [shape((order + u_rows, lanes), BF)] + [shape((2, rank, order), BF)] * 2 + [shape((rank, order), BF)] * 2,
        *in_hbm, space=pltpu.HBM,
        scratch=[
            pltpu.SMEM(ranks.shape, jnp.int32),
            pltpu.VMEM((order, lanes), F32),
            pltpu.VMEM((TURNS, rank, order), BF),
            pltpu.VMEM((slots, slots, TURNS, rank, order), BF),
            pltpu.SemaphoreType.DMA((4,)),
        ],
    )
    near = gather(near)
    v_a, v_b = turn_rows([v_a, v_b])
    later_u = u_here[1].reshape(slots, TURNS * rank, order)
    nxt = gather(jnp.concatenate([inv_here[1].astype(BF)] + [
        later_u[a, :, m * lanes : (m + 1) * lanes] for a in range(slots) for m in range(n_col)], axis=0))

    msg, far_a, far_b = call(
        kernel(first_kernel), [messages, far_shape, far_shape],
        rhs_here, v_a, v_b, later_a, later_b, *near, scratch=[near_scratch],
    )

    rhs_late, inv_late, msg, far_a, far_b = lax.optimization_barrier((rhs_here, inv_here, msg, far_a, far_b))
    later_a, later_b = turn_rows([far_a, far_b])
    far = gather(jnp.stack([later_a, later_b])[:, :, order:])
    same, other = spread(msg)
    z = gather(lax.dot_general(rhs_late, inv_late, (((2,), (1,)), ((0,), (0,))), precision=lax.Precision.HIGHEST,
                               preferred_element_type=F32))

    msg, minus, own = call(
        kernel(middle_kernel),
        [messages, shape((r_cols, order), F32), shape((width + rank - r_cols, r_cols), BF)],
        same, other, rhs_here, later_a, later_b, *far, *nxt,
        scratch=solve_scratch + [pltpu.VMEM((n_col, TURNS, rank, width + rank), BF), next_scratch],
    )
    same, other = spread(msg)
    early, z_last = call(
        kernel(early_kernel), [shape((r_cols, order), F32)] * 2, own, *near, *z,
        scratch=[near_scratch, pltpu.VMEM((n_col, slots, r_cols, lanes), F32)])
    (y,) = call(
        kernel(last_kernel), [shape((slots, r_cols, order), F32)],
        same, other, minus, z_last, early, *nxt, scratch=solve_scratch + [next_scratch],
    )
    return y[:, None]


def solution(mesh):
    n_row, n_col = (mesh.shape[name] for name in ("row", "col"))
    fine = Mesh(mesh.devices.reshape(n_row, n_col // 2, 2), ("row", "x", "core"))
    col = ("x", "core")
    in_specs = (
        P(None, "row", None, None),
        P(None, "row", None, col),
        P(None, "row", None, col, None, None),
        P(None, "row", None, col, None, None),
        P(None, "row", None, col),
    )
    out_specs = P(None, "row", None, None)
    return jax.shard_map(on_device, mesh=fine, in_specs=in_specs, out_specs=out_specs, check_vma=False)
```

```python
import functools

import jax
import jax.numpy as jnp
from jax import lax
from jax.experimental import pallas as pl
from jax.experimental.pallas import tpu as pltpu
from jax.sharding import Mesh
from jax.sharding import PartitionSpec as P

BF = jnp.bfloat16
F32 = jnp.float32
NT = (((1,), (1,)), ((), ()))
TN = (((0,), (0,)), ((), ()))
TURNS = 2


def mm(a, b):
    return jnp.dot(a, b, preferred_element_type=F32)


def split_mm(a, b):
    high = a.astype(BF)
    low = (a - high.astype(F32)).astype(BF)
    return mm(high, b) + mm(low, b)


def pack(low, high, both, half):
    return jnp.concatenate([high[:, :half], jnp.where(both, low[:, :half], high[:, half:])], axis=1)


def place():
    row, x, core = lax.axis_index("row"), lax.axis_index("x"), lax.axis_index("core")
    n_col = lax.axis_size("x") * lax.axis_size("core")
    return row, x * lax.axis_size("core") + core, row // n_col


def join(scratch, pieces):
    x, core, n_x = lax.axis_index("x"), lax.axis_index("core"), lax.axis_size("x")
    for s in range(n_x):
        for other in range(2):
            source = lax.rem(x - s + n_x, n_x) * 2 + (1 - core if other else core)
            scratch[source] = pieces[2 * s + other][...]


def put_columns(out_ref, at, rows, block):
    lanes = out_ref.shape[1]
    count = block.shape[1] // lanes
    for m in range(count):
        out_ref[at + m * rows : at + (m + 1) * rows, :] = block[:, m * lanes : (m + 1) * lanes]


def columns(ref, source, at, rows, start, stop, count):
    return jnp.concatenate([ref[source, at + m * rows + start : at + m * rows + stop, :] for m in range(count)], axis=1)


def prep_kernel(dims, ranks_hbm, inv_hbm, u_hbm, v_hbm, near_ref, send_a_ref, send_b_ref, later_a_ref, later_b_ref,
                ranks_ref, inv_ref, u_ref, v_ref, sems):
    _, _, _, rank, _, _ = dims
    _, _, turn = place()
    order = inv_ref.shape[0]
    copies = [
        pltpu.make_async_copy(inv_hbm.at[0], inv_ref, sems.at[0]),
        pltpu.make_async_copy(u_hbm.at[0, 0], u_ref, sems.at[1]),
        pltpu.make_async_copy(v_hbm, v_ref, sems.at[2]),
        pltpu.make_async_copy(ranks_hbm, ranks_ref, sems.at[3]),
    ]
    for copy in copies:
        copy.start()
    copies[0].wait()
    copies[1].wait()
    near_ref[:order, :] = inv_ref[...].astype(BF)
    put_columns(near_ref, order, TURNS * rank, u_ref[...].reshape(TURNS * rank, order))
    copies[2].wait()
    copies[3].wait()
    rank_rows = lax.broadcasted_iota(jnp.int32, v_ref.shape[3:], 0)

    def masked(i, k, t):
        v = v_ref[i, k, t]
        return jnp.where(rank_rows < ranks_ref[i, 0, 0, k * TURNS + t], v, jnp.zeros_like(v))

    for s, (send_ref, later_ref) in enumerate(((send_a_ref, later_a_ref), (send_b_ref, later_b_ref))):
        t = lax.rem(turn + s, TURNS)
        send_ref[0] = masked(0, 0, t)
        send_ref[1] = masked(1, 0, t)
        later_ref[...] = masked(1, 1, t)


def gathered_inverse(ref, order):
    return jnp.concatenate([ref[c, :order, :] for c in range(ref.shape[0])], axis=1)


def gathered_u(ref, at, rank, blocks):
    n_col = ref.shape[0]
    return jnp.concatenate(
        [columns(ref, j % n_col, at, TURNS * rank, (j // n_col) * rank, (j // n_col + 1) * rank, n_col)
         for j in range(blocks)], axis=0)


def first_kernel(dims, *refs):
    n_row, _, _, rank, width, half = dims
    rhs_ref, v_a_ref, v_b_ref, later_a_ref, later_b_ref = refs[:5]
    msg_ref, far_a_ref, far_b_ref, near_ref = refs[-4:]
    row, col, turn = place()
    order = rhs_ref.shape[2]
    join(near_ref, refs[5:-4])
    inv = gathered_inverse(near_ref, order)
    z = split_mm(rhs_ref[0], inv)
    w = mm(gathered_u(near_ref, order, rank, n_row - 1), inv)
    x = jnp.concatenate([z.astype(BF), w.astype(BF)], axis=0)
    tiles = []
    for v_ref in (v_a_ref, v_b_ref):
        v = v_ref[...].reshape(2 * rank, order)
        tiles.append(lax.dot_general(v, x, NT, preferred_element_type=F32).astype(BF))
    straight = turn == 0
    low = jnp.where(straight, tiles[0][:rank, :width], tiles[1][:rank, :width])
    high = jnp.where(straight, tiles[1][:rank, :width], tiles[0][:rank, :width])
    for n, (far_ref, later_ref) in enumerate(((far_a_ref, later_a_ref), (far_b_ref, later_b_ref))):
        far_ref[:, order : order + width + rank] = tiles[n][rank:]
        far_ref[:, :order] = later_ref[...]
    msg = pack(low, high, col > row, half)
    for d in range(msg_ref.shape[0]):
        msg_ref[d] = msg


def start_solve(q_ref, n_row, r_cols):
    q_ref[...] = jnp.zeros(q_ref.shape, BF)
    eye = (
        lax.broadcasted_iota(jnp.int32, (r_cols, r_cols), 0)
        == lax.broadcasted_iota(jnp.int32, (r_cols, r_cols), 1)
    ).astype(BF)
    for k in range(n_row):
        q_ref[k, :r_cols, :] = eye


def solve(dims, same_ref, other_ref, g_ref, q_ref, c_ref, extra):
    n_row, n_col, r_cols, rank, width, half = dims
    core = lax.axis_index("core")
    g_ref[core] = same_ref[...]
    g_ref[1 - core] = other_ref[...]
    start_solve(q_ref, n_row, r_cols)
    c_ref[...] = jnp.zeros(c_ref.shape, BF)

    def blocks(k):
        w = half if k <= n_col - 2 else width
        parts = []
        for i in range(k + 1, n_row):
            c, t = i % n_col, i // n_col
            at = half if t == 0 else 0
            parts.append(g_ref[c % 2, k * (n_col // 2) + c // 2, :, at : at + w])
        if extra is not None:
            if k == n_row - 1:
                w = width + rank
            parts.append(extra(k)[:, :w])
        return (jnp.concatenate(parts, axis=0) if parts else None), w

    carried = []
    for k in range(0, n_row, 2):
        first, w = blocks(k)
        second, w_next = blocks(k + 1)
        if second is None:
            carried.append(None)
            continue
        at = r_cols + k * rank
        c_ref[k // 2, at : at + rank, :w] = -first[:rank]
        carried.append(mm(second, c_ref[k // 2, :w_next, :w]).astype(BF))

    extras = []
    for k in range(0, n_row, 2):
        first, w = blocks(k)
        second, w_next = blocks(k + 1)
        at = r_cols + k * rank
        q = q_ref[k, :w, :]
        new = mm(first, q)
        if extra is not None:
            extras.append(new[(n_row - 1 - k) * rank :].astype(BF))
        if second is not None:
            later = mm(second, q_ref[k + 1, :w_next, :]) + mm(carried[k // 2], q)
            if extra is not None:
                extras.append(later[(n_row - 2 - k) * rank :].astype(BF))
        q_ref[k + 1, at : at + rank, :] = (-new[:rank]).astype(BF)
        for i in range(k + 2, n_row):
            row = (i - k - 1) * rank
            pair = jnp.concatenate([new[row : row + rank], later[row - rank : row]], axis=0)
            q_ref[i, at : at + 2 * rank, :] = (-pair).astype(BF)
    return extras


def middle_kernel(dims, *refs):
    n_row, n_col, r_cols, rank, _, half = dims
    same_ref, other_ref, rhs_ref, v_a_ref, v_b_ref = refs[:5]
    fars, nexts = refs[5 : 5 + n_col], refs[5 + n_col : 5 + 2 * n_col]
    msg_ref, minus_ref, own_ref, g_ref, q_ref, c_ref, far_ref, next_ref = refs[5 + 2 * n_col :]
    row, col, turn = place()
    order = rhs_ref.shape[2]
    rows = n_col * TURNS * rank
    join(next_ref, nexts)
    join(far_ref, fars)
    inv = gathered_inverse(next_ref, order)
    w = mm(gathered_u(next_ref, order + rows, rank, n_row - 2), inv)
    p = solve(dims, same_ref, other_ref, g_ref, q_ref, c_ref,
              lambda k: far_ref[k % n_col, lax.rem(turn - k // n_col + TURNS, TURNS)])
    total = lax.dot_general(jnp.concatenate(p, axis=0), gathered_u(next_ref, order, rank, n_row), TN,
                            preferred_element_type=F32)
    z = split_mm(rhs_ref[1] - total, inv)
    minus_ref[...] = -total
    x = jnp.concatenate([z.astype(BF), w.astype(BF)], axis=0)
    tiles = [lax.dot_general(v_ref[:, :order], x, NT, preferred_element_type=F32).astype(BF) for v_ref in (v_a_ref, v_b_ref)]
    straight = turn == 0
    low = jnp.where(straight, tiles[0], tiles[1])
    high = jnp.where(straight, tiles[1], tiles[0])
    msg = pack(low, high, col > row, half)
    for d in range(msg_ref.shape[0]):
        msg_ref[d] = msg
    own_ref[...] = q_ref[row][r_cols:, :]


def early_kernel(dims, *refs):
    n_row, n_col, _, rank, _, _ = dims
    own_ref = refs[0]
    nears, zs, nexts = (refs[1 + n * n_col : 1 + (n + 1) * n_col] for n in range(3))
    y_ref, z_out_ref, inv_ref, u_ref, near_ref, z_ref, next_ref = refs[1 + 3 * n_col :]
    order = y_ref.shape[1]
    join(near_ref, nears)
    join(z_ref, zs)
    join(next_ref, nexts)
    minus = lax.dot_general(own_ref[...], gathered_u(near_ref, order, rank, n_row - 1), TN, preferred_element_type=F32)
    z = jnp.concatenate([z_ref[c, 0] for c in range(n_col)], axis=1)
    y_ref[...] = z + split_mm(minus, gathered_inverse(near_ref, order))
    z_out_ref[...] = jnp.concatenate([z_ref[c, 1] for c in range(n_col)], axis=1)
    inv_ref[...] = gathered_inverse(next_ref, order)
    u_ref[...] = gathered_u(next_ref, order + n_col * TURNS * rank, rank, n_row - 1)


def last_kernel(dims, same_ref, other_ref, minus_ref, z_ref, early_ref, inv_ref, u_ref, y_ref, g_ref, q_ref, c_ref):
    y_ref[0] = early_ref[...]
    solve(dims, same_ref, other_ref, g_ref, q_ref, c_ref, None)
    own = q_ref[lax.axis_index("row")][dims[2] :, :]
    minus = minus_ref[...] + lax.dot_general(own, u_ref[...], TN, preferred_element_type=F32)
    y_ref[1] = z_ref[...] + split_mm(minus, inv_ref[...])


def call(kernel, outs, *args, scratch=(), space=pltpu.VMEM):
    return pl.pallas_call(
        kernel,
        out_shape=outs,
        in_specs=[pl.BlockSpec(memory_space=space)] * len(args),
        out_specs=[pl.BlockSpec(memory_space=pltpu.VMEM)] * len(outs),
        scratch_shapes=list(scratch),
        compiler_params=pltpu.CompilerParams(vmem_limit_bytes=24 * 2**20),
    )(*args)


def on_device(rhs, inverse_t, u_factors, v_factors, tile_ranks):
    slots, _, r_cols, order = rhs.shape
    rank = u_factors.shape[4]
    n_row = lax.axis_size("row")
    n_x = lax.axis_size("x")
    n_col = 2 * n_x
    assert slots == 2 and n_row == TURNS * n_col and u_factors.shape[2] == slots * TURNS
    everywhere = ("row", "x", "core")
    lanes = order // n_col
    width = r_cols + (n_row - 2) * rank
    half = r_cols + (n_col - 2) * rank
    assert 2 * half == width
    dims = (n_row, n_col, r_cols, rank, width, half)
    shape = jax.ShapeDtypeStruct
    swap = [(0, 1), (1, 0)]

    rhs_here = rhs[:, 0]
    inv_here = inverse_t[:, 0]
    u_here = u_factors[:, 0, :, 0].reshape(slots, slots, TURNS, rank, order)
    v_here = v_factors[:, 0, :, 0].reshape(slots, slots, TURNS, rank, order)
    ranks = jnp.swapaxes(tile_ranks, 2, 3)

    def gather(part):
        pieces = []
        for s in range(n_x):
            moved = part
            if s:
                moved = lax.ppermute(part, "x", [(i, (i + s) % n_x) for i in range(n_x)])
            pieces += [moved, lax.ppermute(moved, "core", swap)]
        return pieces

    def turn_rows(parts):
        got = []
        for s in range(TURNS):
            pairs = []
            for t in range(TURNS):
                for c in range(n_col):
                    for q in range(n_col):
                        pairs.append(((t * n_col + c) * n_col + q, (((t + s) % TURNS) * n_col + q) * n_col + c))
            got.append(lax.ppermute(parts[s], everywhere, pairs))
        return got

    def spread(m):
        same = lax.all_to_all(m, ("row", "x"), split_axis=0, concat_axis=0, tiled=True)
        return same, lax.ppermute(same, "core", swap)

    def kernel(body):
        return functools.partial(body, dims)

    u_rows = n_col * TURNS * rank
    messages = shape((n_row * n_x, rank, width), BF)
    far_shape = shape((rank, order + width + rank), BF)
    near_scratch = pltpu.VMEM((n_col, order + u_rows, lanes), BF)
    next_scratch = pltpu.VMEM((n_col, order + 2 * u_rows, lanes), BF)
    solve_scratch = [
        pltpu.VMEM((2, n_row * n_x, rank, width), BF),
        pltpu.VMEM((n_row, width + rank, r_cols), BF),
        pltpu.VMEM((n_row // 2, width + rank, width), BF),
    ]

    in_hbm = [pltpu.with_memory_space_constraint(x, pltpu.HBM) for x in (ranks, inv_here, u_here, v_here)]
    near, v_a, v_b, later_a, later_b = call(
        kernel(prep_kernel),
        [shape((order + u_rows, lanes), BF)] + [shape((2, rank, order), BF)] * 2 + [shape((rank, order), BF)] * 2,
        *in_hbm, space=pltpu.HBM,
        scratch=[
            pltpu.SMEM(ranks.shape, jnp.int32),
            pltpu.VMEM((order, lanes), F32),
            pltpu.VMEM((TURNS, rank, order), BF),
            pltpu.VMEM((slots, slots, TURNS, rank, order), BF),
            pltpu.SemaphoreType.DMA((4,)),
        ],
    )
    near = gather(near)
    v_a, v_b = turn_rows([v_a, v_b])
    later_u = u_here[1].reshape(slots, TURNS * rank, order)
    nxt = gather(jnp.concatenate([inv_here[1].astype(BF)] + [
        later_u[a, :, m * lanes : (m + 1) * lanes] for a in range(slots) for m in range(n_col)], axis=0))

    msg, far_a, far_b = call(
        kernel(first_kernel), [messages, far_shape, far_shape],
        rhs_here, v_a, v_b, later_a, later_b, *near, scratch=[near_scratch],
    )

    rhs_late, inv_late, msg, far_a, far_b = lax.optimization_barrier((rhs_here, inv_here, msg, far_a, far_b))
    later_a, later_b = turn_rows([far_a, far_b])
    far = gather(jnp.stack([later_a, later_b])[:, :, order:])
    same, other = spread(msg)
    z = gather(lax.dot_general(rhs_late, inv_late, (((2,), (1,)), ((0,), (0,))), precision=lax.Precision.HIGHEST,
                               preferred_element_type=F32))

    msg, minus, own = call(
        kernel(middle_kernel),
        [messages, shape((r_cols, order), F32), shape((width + rank - r_cols, r_cols), BF)],
        same, other, rhs_here, later_a, later_b, *far, *nxt,
        scratch=solve_scratch + [pltpu.VMEM((n_col, TURNS, rank, width + rank), BF), next_scratch],
    )
    same, other = spread(msg)
    early, z_last, inv_last, u_last = call(
        kernel(early_kernel),
        [shape((r_cols, order), F32)] * 2 + [shape((order, order), BF), shape(((n_row - 1) * rank, order), BF)],
        own, *near, *z, *nxt,
        scratch=[near_scratch, pltpu.VMEM((n_col, slots, r_cols, lanes), F32), next_scratch])
    (y,) = call(
        kernel(last_kernel), [shape((slots, r_cols, order), F32)],
        same, other, minus, z_last, early, inv_last, u_last, scratch=solve_scratch,
    )
    return y[:, None]


def solution(mesh):
    n_row, n_col = (mesh.shape[name] for name in ("row", "col"))
    fine = Mesh(mesh.devices.reshape(n_row, n_col // 2, 2), ("row", "x", "core"))
    col = ("x", "core")
    in_specs = (
        P(None, "row", None, None),
        P(None, "row", None, col),
        P(None, "row", None, col, None, None),
        P(None, "row", None, col, None, None),
        P(None, "row", None, col),
    )
    out_specs = P(None, "row", None, None)
    return jax.shard_map(on_device, mesh=fine, in_specs=in_specs, out_specs=out_specs, check_vma=False)
```

```python
import functools

import jax
import jax.numpy as jnp
from jax import lax
from jax.experimental import pallas as pl
from jax.experimental.pallas import tpu as pltpu
from jax.sharding import Mesh
from jax.sharding import PartitionSpec as P

BF = jnp.bfloat16
F32 = jnp.float32
NT = (((1,), (1,)), ((), ()))
TN = (((0,), (0,)), ((), ()))
TURNS = 2


def mm(a, b):
    return jnp.dot(a, b, preferred_element_type=F32)


def split_mm(a, b):
    high = a.astype(BF)
    low = (a - high.astype(F32)).astype(BF)
    return mm(high, b) + mm(low, b)


def pack(low, high, both, half):
    return jnp.concatenate([high[:, :half], jnp.where(both, low[:, :half], high[:, half:])], axis=1)


def place():
    row, x, core = lax.axis_index("row"), lax.axis_index("x"), lax.axis_index("core")
    n_col = lax.axis_size("x") * lax.axis_size("core")
    return row, x * lax.axis_size("core") + core, row // n_col


def join(scratch, pieces):
    x, core, n_x = lax.axis_index("x"), lax.axis_index("core"), lax.axis_size("x")
    for s in range(n_x):
        for other in range(2):
            source = lax.rem(x - s + n_x, n_x) * 2 + (1 - core if other else core)
            scratch[source] = pieces[2 * s + other][...]


def put_columns(out_ref, at, rows, block):
    lanes = out_ref.shape[1]
    count = block.shape[1] // lanes
    for m in range(count):
        out_ref[at + m * rows : at + (m + 1) * rows, :] = block[:, m * lanes : (m + 1) * lanes]


def columns(ref, source, at, rows, start, stop, count):
    return jnp.concatenate([ref[source, at + m * rows + start : at + m * rows + stop, :] for m in range(count)], axis=1)


def prep_kernel(dims, ranks_hbm, inv_hbm, u_hbm, v_hbm, near_ref, send_a_ref, send_b_ref, later_a_ref, later_b_ref,
                ranks_ref, inv_ref, u_ref, v_ref, sems):
    _, _, _, rank, _, _ = dims
    _, _, turn = place()
    order = inv_ref.shape[0]
    copies = [
        pltpu.make_async_copy(inv_hbm.at[0], inv_ref, sems.at[0]),
        pltpu.make_async_copy(u_hbm.at[0, 0], u_ref, sems.at[1]),
        pltpu.make_async_copy(v_hbm, v_ref, sems.at[2]),
        pltpu.make_async_copy(ranks_hbm, ranks_ref, sems.at[3]),
    ]
    for copy in copies:
        copy.start()
    copies[0].wait()
    copies[1].wait()
    near_ref[:order, :] = inv_ref[...].astype(BF)
    put_columns(near_ref, order, TURNS * rank, u_ref[...].reshape(TURNS * rank, order))
    copies[2].wait()
    copies[3].wait()
    rank_rows = lax.broadcasted_iota(jnp.int32, v_ref.shape[3:], 0)

    def masked(i, k, t):
        v = v_ref[i, k, t]
        return jnp.where(rank_rows < ranks_ref[i, 0, 0, k * TURNS + t], v, jnp.zeros_like(v))

    for s, (send_ref, later_ref) in enumerate(((send_a_ref, later_a_ref), (send_b_ref, later_b_ref))):
        t = lax.rem(turn + s, TURNS)
        send_ref[0] = masked(0, 0, t)
        send_ref[1] = masked(1, 0, t)
        later_ref[...] = masked(1, 1, t)


def gathered_inverse(ref, order):
    return jnp.concatenate([ref[c, :order, :] for c in range(ref.shape[0])], axis=1)


def gathered_u(ref, at, rank, blocks):
    n_col = ref.shape[0]
    return jnp.concatenate(
        [columns(ref, j % n_col, at, TURNS * rank, (j // n_col) * rank, (j // n_col + 1) * rank, n_col)
         for j in range(blocks)], axis=0)


def first_kernel(dims, *refs):
    n_row, _, _, rank, width, half = dims
    rhs_ref, v_a_ref, v_b_ref, later_a_ref, later_b_ref = refs[:5]
    msg_ref, far_a_ref, far_b_ref, near_ref = refs[-4:]
    row, col, turn = place()
    order = rhs_ref.shape[2]
    join(near_ref, refs[5:-4])
    inv = gathered_inverse(near_ref, order)
    z = split_mm(rhs_ref[0], inv)
    w = mm(gathered_u(near_ref, order, rank, n_row - 1), inv)
    x = jnp.concatenate([z.astype(BF), w.astype(BF)], axis=0)
    tiles = []
    for v_ref in (v_a_ref, v_b_ref):
        v = v_ref[...].reshape(2 * rank, order)
        tiles.append(lax.dot_general(v, x, NT, preferred_element_type=F32).astype(BF))
    straight = turn == 0
    low = jnp.where(straight, tiles[0][:rank, :width], tiles[1][:rank, :width])
    high = jnp.where(straight, tiles[1][:rank, :width], tiles[0][:rank, :width])
    for n, (far_ref, later_ref) in enumerate(((far_a_ref, later_a_ref), (far_b_ref, later_b_ref))):
        far_ref[:, order : order + width + rank] = tiles[n][rank:]
        far_ref[:, :order] = later_ref[...]
    msg = pack(low, high, col > row, half)
    for d in range(msg_ref.shape[0]):
        msg_ref[d] = msg


def start_solve(q_ref, n_row, r_cols):
    q_ref[...] = jnp.zeros(q_ref.shape, BF)
    eye = (
        lax.broadcasted_iota(jnp.int32, (r_cols, r_cols), 0)
        == lax.broadcasted_iota(jnp.int32, (r_cols, r_cols), 1)
    ).astype(BF)
    for k in range(n_row):
        q_ref[k, :r_cols, :] = eye


def solve(dims, same_ref, other_ref, g_ref, q_ref, c_ref, extra):
    n_row, n_col, r_cols, rank, width, half = dims
    core = lax.axis_index("core")
    g_ref[core] = same_ref[...]
    g_ref[1 - core] = other_ref[...]
    start_solve(q_ref, n_row, r_cols)
    c_ref[...] = jnp.zeros(c_ref.shape, BF)

    def blocks(k):
        w = half if k <= n_col - 2 else width
        parts = []
        for i in range(k + 1, n_row):
            c, t = i % n_col, i // n_col
            at = half if t == 0 else 0
            parts.append(g_ref[c % 2, k * (n_col // 2) + c // 2, :, at : at + w])
        if extra is not None:
            if k == n_row - 1:
                w = width + rank
            parts.append(extra(k)[:, :w])
        return (jnp.concatenate(parts, axis=0) if parts else None), w

    carried = []
    for k in range(0, n_row, 2):
        first, w = blocks(k)
        second, w_next = blocks(k + 1)
        if second is None:
            carried.append(None)
            continue
        at = r_cols + k * rank
        c_ref[k // 2, at : at + rank, :w] = -first[:rank]
        carried.append(mm(second, c_ref[k // 2, :w_next, :w]).astype(BF))

    extras = []
    for k in range(0, n_row, 2):
        first, w = blocks(k)
        second, w_next = blocks(k + 1)
        at = r_cols + k * rank
        q = q_ref[k, :w, :]
        new = mm(first, q)
        if extra is not None:
            extras.append(new[(n_row - 1 - k) * rank :].astype(BF))
        if second is not None:
            later = mm(second, q_ref[k + 1, :w_next, :]) + mm(carried[k // 2], q)
            if extra is not None:
                extras.append(later[(n_row - 2 - k) * rank :].astype(BF))
        q_ref[k + 1, at : at + rank, :] = (-new[:rank]).astype(BF)
        for i in range(k + 2, n_row):
            row = (i - k - 1) * rank
            pair = jnp.concatenate([new[row : row + rank], later[row - rank : row]], axis=0)
            q_ref[i, at : at + 2 * rank, :] = (-pair).astype(BF)
    return extras


def ready_kernel(dims, *refs):
    n_row, n_col, r_cols, rank, _, _ = dims
    v_a_ref, v_b_ref = refs[:2]
    fars, nexts = refs[2 : 2 + n_col], refs[2 + n_col : 2 + 2 * n_col]
    far_ref, inv_ref, u_low_ref, u_ref, m_ref, next_ref = refs[2 + 2 * n_col :]
    _, _, turn = place()
    order = inv_ref.shape[1]
    rows = n_col * TURNS * rank
    join(next_ref, nexts)
    join(far_ref, fars)
    inv = gathered_inverse(next_ref, order)
    inv_ref[...] = inv
    u_low_ref[...] = gathered_u(next_ref, order, rank, n_row)
    u = gathered_u(next_ref, order + rows, rank, n_row - 1)
    u_ref[...] = u
    w = mm(u[: (n_row - 2) * rank], inv)
    x = jnp.concatenate([jnp.zeros((r_cols, order), BF), w.astype(BF)], axis=0)
    tiles = [lax.dot_general(v_ref[:, :order], x, NT, preferred_element_type=F32).astype(BF)
             for v_ref in (v_a_ref, v_b_ref)]
    straight = turn == 0
    m_ref[0] = jnp.where(straight, tiles[0], tiles[1])
    m_ref[1] = jnp.where(straight, tiles[1], tiles[0])


def middle_kernel(dims, same_ref, other_ref, rhs_ref, v_a_ref, v_b_ref, far_ref, inv_ref, u_low_ref, m_ref,
                  msg_ref, minus_ref, own_ref, g_ref, q_ref, c_ref):
    _, n_col, r_cols, _, _, half = dims
    row, col, turn = place()
    order = rhs_ref.shape[2]
    p = solve(dims, same_ref, other_ref, g_ref, q_ref, c_ref,
              lambda k: far_ref[k % n_col, lax.rem(turn - k // n_col + TURNS, TURNS)])
    total = lax.dot_general(jnp.concatenate(p, axis=0), u_low_ref[...], TN, preferred_element_type=F32)
    z = split_mm(rhs_ref[1] - total, inv_ref[...])
    minus_ref[...] = -total
    x = jnp.concatenate([z.astype(BF), jnp.zeros((half - r_cols, order), BF)], axis=0)
    tiles = [lax.dot_general(v_ref[:, :order], x, NT, preferred_element_type=F32).astype(BF)
             for v_ref in (v_a_ref, v_b_ref)]
    straight = turn == 0
    low = m_ref[0, :, :half] + jnp.where(straight, tiles[0], tiles[1])
    high = m_ref[1, :, :half] + jnp.where(straight, tiles[1], tiles[0])
    msg = jnp.concatenate([high, jnp.where(col > row, low, m_ref[1, :, half:])], axis=1)
    for d in range(msg_ref.shape[0]):
        msg_ref[d] = msg
    own_ref[...] = q_ref[row][r_cols:, :]


def early_kernel(dims, *refs):
    n_row, n_col, _, rank, _, _ = dims
    own_ref = refs[0]
    nears, zs = refs[1 : 1 + n_col], refs[1 + n_col : 1 + 2 * n_col]
    y_ref, z_out_ref, near_ref, z_ref = refs[1 + 2 * n_col :]
    order = y_ref.shape[1]
    join(near_ref, nears)
    join(z_ref, zs)
    minus = lax.dot_general(own_ref[...], gathered_u(near_ref, order, rank, n_row - 1), TN, preferred_element_type=F32)
    z = jnp.concatenate([z_ref[c, 0] for c in range(n_col)], axis=1)
    y_ref[...] = z + split_mm(minus, gathered_inverse(near_ref, order))
    z_out_ref[...] = jnp.concatenate([z_ref[c, 1] for c in range(n_col)], axis=1)


def last_kernel(dims, same_ref, other_ref, minus_ref, z_ref, early_ref, inv_ref, u_ref, y_ref, g_ref, q_ref, c_ref):
    y_ref[0] = early_ref[...]
    solve(dims, same_ref, other_ref, g_ref, q_ref, c_ref, None)
    own = q_ref[lax.axis_index("row")][dims[2] :, :]
    minus = minus_ref[...] + lax.dot_general(own, u_ref[...], TN, preferred_element_type=F32)
    y_ref[1] = z_ref[...] + split_mm(minus, inv_ref[...])


def call(kernel, outs, *args, scratch=(), space=pltpu.VMEM):
    return pl.pallas_call(
        kernel,
        out_shape=outs,
        in_specs=[pl.BlockSpec(memory_space=space)] * len(args),
        out_specs=[pl.BlockSpec(memory_space=pltpu.VMEM)] * len(outs),
        scratch_shapes=list(scratch),
        compiler_params=pltpu.CompilerParams(vmem_limit_bytes=24 * 2**20),
    )(*args)


def on_device(rhs, inverse_t, u_factors, v_factors, tile_ranks):
    slots, _, r_cols, order = rhs.shape
    rank = u_factors.shape[4]
    n_row = lax.axis_size("row")
    n_x = lax.axis_size("x")
    n_col = 2 * n_x
    assert slots == 2 and n_row == TURNS * n_col and u_factors.shape[2] == slots * TURNS
    everywhere = ("row", "x", "core")
    lanes = order // n_col
    width = r_cols + (n_row - 2) * rank
    half = r_cols + (n_col - 2) * rank
    assert 2 * half == width
    dims = (n_row, n_col, r_cols, rank, width, half)
    shape = jax.ShapeDtypeStruct
    swap = [(0, 1), (1, 0)]

    rhs_here = rhs[:, 0]
    inv_here = inverse_t[:, 0]
    u_here = u_factors[:, 0, :, 0].reshape(slots, slots, TURNS, rank, order)
    v_here = v_factors[:, 0, :, 0].reshape(slots, slots, TURNS, rank, order)
    ranks = jnp.swapaxes(tile_ranks, 2, 3)

    def gather(part):
        pieces = []
        for s in range(n_x):
            moved = part
            if s:
                moved = lax.ppermute(part, "x", [(i, (i + s) % n_x) for i in range(n_x)])
            pieces += [moved, lax.ppermute(moved, "core", swap)]
        return pieces

    def turn_rows(parts):
        got = []
        for s in range(TURNS):
            pairs = []
            for t in range(TURNS):
                for c in range(n_col):
                    for q in range(n_col):
                        pairs.append(((t * n_col + c) * n_col + q, (((t + s) % TURNS) * n_col + q) * n_col + c))
            got.append(lax.ppermute(parts[s], everywhere, pairs))
        return got

    def spread(m):
        same = lax.all_to_all(m, ("row", "x"), split_axis=0, concat_axis=0, tiled=True)
        return same, lax.ppermute(same, "core", swap)

    def kernel(body):
        return functools.partial(body, dims)

    u_rows = n_col * TURNS * rank
    messages = shape((n_row * n_x, rank, width), BF)
    far_shape = shape((rank, order + width + rank), BF)
    near_scratch = pltpu.VMEM((n_col, order + u_rows, lanes), BF)
    next_scratch = pltpu.VMEM((n_col, order + 2 * u_rows, lanes), BF)
    solve_scratch = [
        pltpu.VMEM((2, n_row * n_x, rank, width), BF),
        pltpu.VMEM((n_row, width + rank, r_cols), BF),
        pltpu.VMEM((n_row // 2, width + rank, width), BF),
    ]

    in_hbm = [pltpu.with_memory_space_constraint(x, pltpu.HBM) for x in (ranks, inv_here, u_here, v_here)]
    near, v_a, v_b, later_a, later_b = call(
        kernel(prep_kernel),
        [shape((order + u_rows, lanes), BF)] + [shape((2, rank, order), BF)] * 2 + [shape((rank, order), BF)] * 2,
        *in_hbm, space=pltpu.HBM,
        scratch=[
            pltpu.SMEM(ranks.shape, jnp.int32),
            pltpu.VMEM((order, lanes), F32),
            pltpu.VMEM((TURNS, rank, order), BF),
            pltpu.VMEM((slots, slots, TURNS, rank, order), BF),
            pltpu.SemaphoreType.DMA((4,)),
        ],
    )
    near = gather(near)
    v_a, v_b = turn_rows([v_a, v_b])
    later_u = u_here[1].reshape(slots, TURNS * rank, order)
    nxt = gather(jnp.concatenate([inv_here[1].astype(BF)] + [
        later_u[a, :, m * lanes : (m + 1) * lanes] for a in range(slots) for m in range(n_col)], axis=0))

    msg, far_a, far_b = call(
        kernel(first_kernel), [messages, far_shape, far_shape],
        rhs_here, v_a, v_b, later_a, later_b, *near, scratch=[near_scratch],
    )

    rhs_late, inv_late, msg, far_a, far_b = lax.optimization_barrier((rhs_here, inv_here, msg, far_a, far_b))
    later_a, later_b = turn_rows([far_a, far_b])
    far = gather(jnp.stack([later_a, later_b])[:, :, order:])
    same, other = spread(msg)
    z = gather(lax.dot_general(rhs_late, inv_late, (((2,), (1,)), ((0,), (0,))), precision=lax.Precision.HIGHEST,
                               preferred_element_type=F32))

    far, inv_next, u_low, u_next, m_next = call(
        kernel(ready_kernel),
        [
            shape((n_col, TURNS, rank, width + rank), BF),
            shape((order, order), BF),
            shape((n_row * rank, order), BF),
            shape(((n_row - 1) * rank, order), BF),
            shape((TURNS, rank, width), BF),
        ],
        later_a, later_b, *far, *nxt, scratch=[next_scratch],
    )
    msg, minus, own = call(
        kernel(middle_kernel),
        [messages, shape((r_cols, order), F32), shape((width + rank - r_cols, r_cols), BF)],
        same, other, rhs_here, later_a, later_b, far, inv_next, u_low, m_next, scratch=solve_scratch,
    )
    same, other = spread(msg)
    early, z_last = call(
        kernel(early_kernel), [shape((r_cols, order), F32)] * 2, own, *near, *z,
        scratch=[near_scratch, pltpu.VMEM((n_col, slots, r_cols, lanes), F32)])
    (y,) = call(
        kernel(last_kernel), [shape((slots, r_cols, order), F32)],
        same, other, minus, z_last, early, inv_next, u_next, scratch=solve_scratch,
    )
    return y[:, None]


def solution(mesh):
    n_row, n_col = (mesh.shape[name] for name in ("row", "col"))
    fine = Mesh(mesh.devices.reshape(n_row, n_col // 2, 2), ("row", "x", "core"))
    col = ("x", "core")
    in_specs = (
        P(None, "row", None, None),
        P(None, "row", None, col),
        P(None, "row", None, col, None, None),
        P(None, "row", None, col, None, None),
        P(None, "row", None, col),
    )
    out_specs = P(None, "row", None, None)
    return jax.shard_map(on_device, mesh=fine, in_specs=in_specs, out_specs=out_specs, check_vma=False)
```

```python
import functools

import jax
import jax.numpy as jnp
from jax import lax
from jax.experimental import pallas as pl
from jax.experimental.pallas import tpu as pltpu
from jax.sharding import Mesh
from jax.sharding import PartitionSpec as P

BF = jnp.bfloat16
F32 = jnp.float32
NT = (((1,), (1,)), ((), ()))
TN = (((0,), (0,)), ((), ()))
TURNS = 2


def mm(a, b):
    return jnp.dot(a, b, preferred_element_type=F32)


def split_mm(a, b):
    high = a.astype(BF)
    low = (a - high.astype(F32)).astype(BF)
    return mm(high, b) + mm(low, b)


def pack(low, high, both, half):
    return jnp.concatenate([high[:, :half], jnp.where(both, low[:, :half], high[:, half:])], axis=1)


def place():
    row, x, core = lax.axis_index("row"), lax.axis_index("x"), lax.axis_index("core")
    n_col = lax.axis_size("x") * lax.axis_size("core")
    return row, x * lax.axis_size("core") + core, row // n_col


def join(scratch, pieces):
    x, core, n_x = lax.axis_index("x"), lax.axis_index("core"), lax.axis_size("x")
    for s in range(n_x):
        for other in range(2):
            source = lax.rem(x - s + n_x, n_x) * 2 + (1 - core if other else core)
            scratch[source] = pieces[2 * s + other][...]


def put_columns(out_ref, at, rows, block):
    lanes = out_ref.shape[1]
    count = block.shape[1] // lanes
    for m in range(count):
        out_ref[at + m * rows : at + (m + 1) * rows, :] = block[:, m * lanes : (m + 1) * lanes]


def columns(ref, source, at, rows, start, stop, count):
    return jnp.concatenate([ref[source, at + m * rows + start : at + m * rows + stop, :] for m in range(count)], axis=1)


def prep_kernel(dims, ranks_hbm, inv_hbm, u_hbm, v_hbm, near_ref, send_a_ref, send_b_ref, later_a_ref, later_b_ref,
                ranks_ref, inv_ref, u_ref, v_ref, sems):
    _, _, _, rank, _, _ = dims
    _, _, turn = place()
    order = inv_ref.shape[0]
    copies = [
        pltpu.make_async_copy(inv_hbm.at[0], inv_ref, sems.at[0]),
        pltpu.make_async_copy(u_hbm.at[0, 0], u_ref, sems.at[1]),
        pltpu.make_async_copy(v_hbm, v_ref, sems.at[2]),
        pltpu.make_async_copy(ranks_hbm, ranks_ref, sems.at[3]),
    ]
    for copy in copies:
        copy.start()
    copies[0].wait()
    copies[1].wait()
    near_ref[:order, :] = inv_ref[...].astype(BF)
    put_columns(near_ref, order, TURNS * rank, u_ref[...].reshape(TURNS * rank, order))
    copies[2].wait()
    copies[3].wait()
    rank_rows = lax.broadcasted_iota(jnp.int32, v_ref.shape[3:], 0)

    def masked(i, k, t):
        v = v_ref[i, k, t]
        return jnp.where(rank_rows < ranks_ref[i, 0, 0, k * TURNS + t], v, jnp.zeros_like(v))

    for s, (send_ref, later_ref) in enumerate(((send_a_ref, later_a_ref), (send_b_ref, later_b_ref))):
        t = lax.rem(turn + s, TURNS)
        send_ref[0] = masked(0, 0, t)
        send_ref[1] = masked(1, 0, t)
        later_ref[...] = masked(1, 1, t)


def gathered_inverse(ref, order):
    return jnp.concatenate([ref[c, :order, :] for c in range(ref.shape[0])], axis=1)


def gathered_u(ref, at, rank, blocks):
    n_col = ref.shape[0]
    return jnp.concatenate(
        [columns(ref, j % n_col, at, TURNS * rank, (j // n_col) * rank, (j // n_col + 1) * rank, n_col)
         for j in range(blocks)], axis=0)


def rows_kernel(dims, rhs_ref, *refs):
    n_row, n_col, r_cols, rank, _, _ = dims
    x_ref, inv_ref, u_ref, near_ref = refs[n_col:]
    order = rhs_ref.shape[2]
    join(near_ref, refs[:n_col])
    inv = gathered_inverse(near_ref, order)
    u = gathered_u(near_ref, order, rank, n_row - 1)
    inv_ref[...] = inv
    u_ref[...] = u
    x_ref[:r_cols, :] = split_mm(rhs_ref[0], inv).astype(BF)
    x_ref[r_cols:, :] = mm(u, inv).astype(BF)


def first_kernel(dims, x_ref, v_a_ref, v_b_ref, later_a_ref, later_b_ref, msg_ref, far_a_ref, far_b_ref):
    _, _, _, rank, width, half = dims
    row, col, turn = place()
    order = x_ref.shape[1]
    x = x_ref[...]
    tiles = []
    for v_ref in (v_a_ref, v_b_ref):
        v = v_ref[...].reshape(2 * rank, order)
        tiles.append(lax.dot_general(v, x, NT, preferred_element_type=F32).astype(BF))
    straight = turn == 0
    low = jnp.where(straight, tiles[0][:rank, :width], tiles[1][:rank, :width])
    high = jnp.where(straight, tiles[1][:rank, :width], tiles[0][:rank, :width])
    for n, (far_ref, later_ref) in enumerate(((far_a_ref, later_a_ref), (far_b_ref, later_b_ref))):
        far_ref[:, order : order + width + rank] = tiles[n][rank:]
        far_ref[:, :order] = later_ref[...]
    msg = pack(low, high, col > row, half)
    for d in range(msg_ref.shape[0]):
        msg_ref[d] = msg


def start_solve(q_ref, n_row, r_cols):
    q_ref[...] = jnp.zeros(q_ref.shape, BF)
    eye = (
        lax.broadcasted_iota(jnp.int32, (r_cols, r_cols), 0)
        == lax.broadcasted_iota(jnp.int32, (r_cols, r_cols), 1)
    ).astype(BF)
    for k in range(n_row):
        q_ref[k, :r_cols, :] = eye


def solve(dims, same_ref, other_ref, g_ref, q_ref, c_ref, extra):
    n_row, n_col, r_cols, rank, width, half = dims
    core = lax.axis_index("core")
    g_ref[core] = same_ref[...]
    g_ref[1 - core] = other_ref[...]
    start_solve(q_ref, n_row, r_cols)
    c_ref[...] = jnp.zeros(c_ref.shape, BF)

    def blocks(k):
        w = half if k <= n_col - 2 else width
        parts = []
        for i in range(k + 1, n_row):
            c, t = i % n_col, i // n_col
            at = half if t == 0 else 0
            parts.append(g_ref[c % 2, k * (n_col // 2) + c // 2, :, at : at + w])
        if extra is not None:
            if k == n_row - 1:
                w = width + rank
            parts.append(extra(k)[:, :w])
        return (jnp.concatenate(parts, axis=0) if parts else None), w

    carried = []
    for k in range(0, n_row, 2):
        first, w = blocks(k)
        second, w_next = blocks(k + 1)
        if second is None:
            carried.append(None)
            continue
        at = r_cols + k * rank
        c_ref[k // 2, at : at + rank, :w] = -first[:rank]
        carried.append(mm(second, c_ref[k // 2, :w_next, :w]).astype(BF))

    extras = []
    for k in range(0, n_row, 2):
        first, w = blocks(k)
        second, w_next = blocks(k + 1)
        at = r_cols + k * rank
        q = q_ref[k, :w, :]
        new = mm(first, q)
        if extra is not None:
            extras.append(new[(n_row - 1 - k) * rank :].astype(BF))
        if second is not None:
            later = mm(second, q_ref[k + 1, :w_next, :]) + mm(carried[k // 2], q)
            if extra is not None:
                extras.append(later[(n_row - 2 - k) * rank :].astype(BF))
        q_ref[k + 1, at : at + rank, :] = (-new[:rank]).astype(BF)
        for i in range(k + 2, n_row):
            row = (i - k - 1) * rank
            pair = jnp.concatenate([new[row : row + rank], later[row - rank : row]], axis=0)
            q_ref[i, at : at + 2 * rank, :] = (-pair).astype(BF)
    return extras


def ready_kernel(dims, *refs):
    n_row, n_col, r_cols, rank, _, _ = dims
    v_a_ref, v_b_ref = refs[:2]
    fars, nexts = refs[2 : 2 + n_col], refs[2 + n_col : 2 + 2 * n_col]
    far_ref, inv_ref, u_low_ref, u_ref, m_ref, next_ref = refs[2 + 2 * n_col :]
    _, _, turn = place()
    order = inv_ref.shape[1]
    rows = n_col * TURNS * rank
    join(next_ref, nexts)
    join(far_ref, fars)
    inv = gathered_inverse(next_ref, order)
    inv_ref[...] = inv
    u_low_ref[...] = gathered_u(next_ref, order, rank, n_row)
    u = gathered_u(next_ref, order + rows, rank, n_row - 1)
    u_ref[...] = u
    w = mm(u[: (n_row - 2) * rank], inv)
    x = jnp.concatenate([jnp.zeros((r_cols, order), BF), w.astype(BF)], axis=0)
    tiles = [lax.dot_general(v_ref[:, :order], x, NT, preferred_element_type=F32).astype(BF)
             for v_ref in (v_a_ref, v_b_ref)]
    straight = turn == 0
    m_ref[0] = jnp.where(straight, tiles[0], tiles[1])
    m_ref[1] = jnp.where(straight, tiles[1], tiles[0])


def middle_kernel(dims, same_ref, other_ref, rhs_ref, v_a_ref, v_b_ref, far_ref, inv_ref, u_low_ref, m_ref,
                  msg_ref, minus_ref, own_ref, g_ref, q_ref, c_ref):
    _, n_col, r_cols, _, _, half = dims
    row, col, turn = place()
    order = rhs_ref.shape[2]
    p = solve(dims, same_ref, other_ref, g_ref, q_ref, c_ref,
              lambda k: far_ref[k % n_col, lax.rem(turn - k // n_col + TURNS, TURNS)])
    total = lax.dot_general(jnp.concatenate(p, axis=0), u_low_ref[...], TN, preferred_element_type=F32)
    z = split_mm(rhs_ref[1] - total, inv_ref[...])
    minus_ref[...] = -total
    x = jnp.concatenate([z.astype(BF), jnp.zeros((half - r_cols, order), BF)], axis=0)
    tiles = [lax.dot_general(v_ref[:, :order], x, NT, preferred_element_type=F32).astype(BF)
             for v_ref in (v_a_ref, v_b_ref)]
    straight = turn == 0
    low = m_ref[0, :, :half] + jnp.where(straight, tiles[0], tiles[1])
    high = m_ref[1, :, :half] + jnp.where(straight, tiles[1], tiles[0])
    msg = jnp.concatenate([high, jnp.where(col > row, low, m_ref[1, :, half:])], axis=1)
    for d in range(msg_ref.shape[0]):
        msg_ref[d] = msg
    own_ref[...] = q_ref[row][r_cols:, :]


def early_kernel(dims, *refs):
    _, n_col, _, _, _, _ = dims
    own_ref, inv_ref, u_ref = refs[:3]
    y_ref, z_out_ref, z_ref = refs[3 + n_col :]
    join(z_ref, refs[3 : 3 + n_col])
    minus = lax.dot_general(own_ref[...], u_ref[...], TN, preferred_element_type=F32)
    z = jnp.concatenate([z_ref[c, 0] for c in range(n_col)], axis=1)
    y_ref[...] = z + split_mm(minus, inv_ref[...])
    z_out_ref[...] = jnp.concatenate([z_ref[c, 1] for c in range(n_col)], axis=1)


def last_kernel(dims, same_ref, other_ref, minus_ref, z_ref, early_ref, inv_ref, u_ref, y_hbm,
                g_ref, q_ref, c_ref, late_ref, sems):
    first_out = pltpu.make_async_copy(early_ref, y_hbm.at[0], sems.at[0])
    first_out.start()
    solve(dims, same_ref, other_ref, g_ref, q_ref, c_ref, None)
    own = q_ref[lax.axis_index("row")][dims[2] :, :]
    minus = minus_ref[...] + lax.dot_general(own, u_ref[...], TN, preferred_element_type=F32)
    late_ref[...] = z_ref[...] + split_mm(minus, inv_ref[...])
    second_out = pltpu.make_async_copy(late_ref, y_hbm.at[1], sems.at[1])
    second_out.start()
    first_out.wait()
    second_out.wait()


def call(kernel, outs, *args, scratch=(), space=pltpu.VMEM, out_space=pltpu.VMEM):
    return pl.pallas_call(
        kernel,
        out_shape=outs,
        in_specs=[pl.BlockSpec(memory_space=space)] * len(args),
        out_specs=[pl.BlockSpec(memory_space=out_space)] * len(outs),
        scratch_shapes=list(scratch),
        compiler_params=pltpu.CompilerParams(vmem_limit_bytes=24 * 2**20),
    )(*args)


def on_device(rhs, inverse_t, u_factors, v_factors, tile_ranks):
    slots, _, r_cols, order = rhs.shape
    rank = u_factors.shape[4]
    n_row = lax.axis_size("row")
    n_x = lax.axis_size("x")
    n_col = 2 * n_x
    assert slots == 2 and n_row == TURNS * n_col and u_factors.shape[2] == slots * TURNS
    everywhere = ("row", "x", "core")
    lanes = order // n_col
    width = r_cols + (n_row - 2) * rank
    half = r_cols + (n_col - 2) * rank
    assert 2 * half == width
    dims = (n_row, n_col, r_cols, rank, width, half)
    shape = jax.ShapeDtypeStruct
    swap = [(0, 1), (1, 0)]

    rhs_here = rhs[:, 0]
    inv_here = inverse_t[:, 0]
    u_here = u_factors[:, 0, :, 0].reshape(slots, slots, TURNS, rank, order)
    v_here = v_factors[:, 0, :, 0].reshape(slots, slots, TURNS, rank, order)
    ranks = jnp.swapaxes(tile_ranks, 2, 3)

    def gather(part):
        pieces = []
        for s in range(n_x):
            moved = part
            if s:
                moved = lax.ppermute(part, "x", [(i, (i + s) % n_x) for i in range(n_x)])
            pieces += [moved, lax.ppermute(moved, "core", swap)]
        return pieces

    def turn_rows(parts):
        got = []
        for s in range(TURNS):
            pairs = []
            for t in range(TURNS):
                for c in range(n_col):
                    for q in range(n_col):
                        pairs.append(((t * n_col + c) * n_col + q, (((t + s) % TURNS) * n_col + q) * n_col + c))
            got.append(lax.ppermute(parts[s], everywhere, pairs))
        return got

    def spread(m):
        same = lax.all_to_all(m, ("row", "x"), split_axis=0, concat_axis=0, tiled=True)
        return same, lax.ppermute(same, "core", swap)

    def kernel(body):
        return functools.partial(body, dims)

    u_rows = n_col * TURNS * rank
    messages = shape((n_row * n_x, rank, width), BF)
    far_shape = shape((rank, order + width + rank), BF)
    near_scratch = pltpu.VMEM((n_col, order + u_rows, lanes), BF)
    next_scratch = pltpu.VMEM((n_col, order + 2 * u_rows, lanes), BF)
    solve_scratch = [
        pltpu.VMEM((2, n_row * n_x, rank, width), BF),
        pltpu.VMEM((n_row, width + rank, r_cols), BF),
        pltpu.VMEM((n_row // 2, width + rank, width), BF),
    ]

    in_hbm = [pltpu.with_memory_space_constraint(x, pltpu.HBM) for x in (ranks, inv_here, u_here, v_here)]
    near, v_a, v_b, later_a, later_b = call(
        kernel(prep_kernel),
        [shape((order + u_rows, lanes), BF)] + [shape((2, rank, order), BF)] * 2 + [shape((rank, order), BF)] * 2,
        *in_hbm, space=pltpu.HBM,
        scratch=[
            pltpu.SMEM(ranks.shape, jnp.int32),
            pltpu.VMEM((order, lanes), F32),
            pltpu.VMEM((TURNS, rank, order), BF),
            pltpu.VMEM((slots, slots, TURNS, rank, order), BF),
            pltpu.SemaphoreType.DMA((4,)),
        ],
    )
    near = gather(near)
    v_a, v_b = turn_rows([v_a, v_b])
    later_u = u_here[1].reshape(slots, TURNS * rank, order)
    nxt = gather(jnp.concatenate([inv_here[1].astype(BF)] + [
        later_u[a, :, m * lanes : (m + 1) * lanes] for a in range(slots) for m in range(n_col)], axis=0))

    x_rows, inv_near, u_near = call(
        kernel(rows_kernel),
        [shape((width + rank, order), BF), shape((order, order), BF), shape(((n_row - 1) * rank, order), BF)],
        rhs_here, *near, scratch=[near_scratch],
    )
    msg, far_a, far_b = call(
        kernel(first_kernel), [messages, far_shape, far_shape],
        x_rows, v_a, v_b, later_a, later_b,
    )

    rhs_late, inv_late, msg, far_a, far_b = lax.optimization_barrier((rhs_here, inv_here, msg, far_a, far_b))
    later_a, later_b = turn_rows([far_a, far_b])
    far = gather(jnp.stack([later_a, later_b])[:, :, order:])
    same, other = spread(msg)
    z = gather(lax.dot_general(rhs_late, inv_late, (((2,), (1,)), ((0,), (0,))), precision=lax.Precision.HIGHEST,
                               preferred_element_type=F32))

    far, inv_next, u_low, u_next, m_next = call(
        kernel(ready_kernel),
        [
            shape((n_col, TURNS, rank, width + rank), BF),
            shape((order, order), BF),
            shape((n_row * rank, order), BF),
            shape(((n_row - 1) * rank, order), BF),
            shape((TURNS, rank, width), BF),
        ],
        later_a, later_b, *far, *nxt, scratch=[next_scratch],
    )
    msg, minus, own = call(
        kernel(middle_kernel),
        [messages, shape((r_cols, order), F32), shape((width + rank - r_cols, r_cols), BF)],
        same, other, rhs_here, later_a, later_b, far, inv_next, u_low, m_next, scratch=solve_scratch,
    )
    same, other = spread(msg)
    early, z_last = call(
        kernel(early_kernel), [shape((r_cols, order), F32)] * 2, own, inv_near, u_near, *z,
        scratch=[pltpu.VMEM((n_col, slots, r_cols, lanes), F32)])
    (y,) = call(
        kernel(last_kernel), [shape((slots, r_cols, order), F32)],
        same, other, minus, z_last, early, inv_next, u_next, out_space=pltpu.HBM,
        scratch=solve_scratch + [pltpu.VMEM((r_cols, order), F32), pltpu.SemaphoreType.DMA((2,))],
    )
    return y[:, None]


def solution(mesh):
    n_row, n_col = (mesh.shape[name] for name in ("row", "col"))
    fine = Mesh(mesh.devices.reshape(n_row, n_col // 2, 2), ("row", "x", "core"))
    col = ("x", "core")
    in_specs = (
        P(None, "row", None, None),
        P(None, "row", None, col),
        P(None, "row", None, col, None, None),
        P(None, "row", None, col, None, None),
        P(None, "row", None, col),
    )
    out_specs = P(None, "row", None, None)
    return jax.shard_map(on_device, mesh=fine, in_specs=in_specs, out_specs=out_specs, check_vma=False)
```
